32 devices in a mesh: lon: 8 (over y, x, core), lat: 4 (over z).
Axes of the slice: x: 2, y: 2, z: 4, core: 2. Of those that a mesh axis runs over, the one named last changes fastest.
Arguments:
- fields: bfloat16 [96, 192, 3, 512], P('lat', 'lon'), may hold values from -6 to 6
- region_ids: int32 [96], P('lat'), may hold values from 0 to 15, never falling along the last dimension, each value on 1 to 12 neighbouring positions
- w_qkv: bfloat16 [1536, 512], P(('lon', 'lat')), may hold values from -2 to 2
- w_proj: bfloat16 [512, 512], P(('lon', 'lat')), may hold values from -0.25 to 0.25
- grad_output: bfloat16 [96, 192, 3, 512], P('lat', 'lon'), may hold values from -6 to 6
Outputs:
- block_out: bfloat16 [96, 192, 3, 512], P('lat', 'lon')
- grad_fields: bfloat16 [96, 192, 3, 512], P('lat', 'lon')
- grad_w_qkv: float32 [1536, 512], P(('lon', 'lat'))
- grad_w_proj: float32 [512, 512], P(('lon', 'lat'))
The draws below stay inside these ranges and needn't reach their ends.
Inputs may be any that keep to these rules, and one draw needn't show every extreme that they name: `region_ids`: region ids never fall along the rows; each region spans 1 to 12 rows.
All inputs are finite; a program needn't handle non-finite values.
Results may differ from the reference program's by a relative error of at most 0.018.
The reference program's roundings to bfloat16 on the way count: a program that leaves them out, or rounds other values in their place, can miss the bound.
Values may be sent and summed in bfloat16 or wider, within the bound.
No kernel may reach another device: no remote copies, remote signals or barrier semaphores. Data moves between devices by JAX's collectives and lax.ppermute only.
A program may use at most 128 MiB of HBM per device.

```python
import math
import jax
import jax.numpy as jnp
import numpy as np
from jax import lax

C = 512
HEADS = 8
HEAD = 64
WIN = 12
LEVELS = 3
NLAT = 96
NLON = 192
TOKENS = 55296


def draw_fields(key, part):
    shape = (NLAT, NLON, LEVELS, C)
    values = jnp.clip(jax.random.normal(jax.random.fold_in(key, 12), shape, jnp.float32), -6.0, 6.0)
    return values.astype(jnp.bfloat16)


def draw_w_qkv(key, part):
    first = jax.random.fold_in(jax.random.fold_in(key, 21), 0)
    whole = jnp.clip(jax.random.normal(first, (3 * C, C), jnp.float32), -6.0, 6.0) * C ** (-0.5)
    return whole.astype(jnp.bfloat16)


def with_spikes(values, stream_key, source, target, blocks, factor):
    owner, partner = [(jnp.arange(values.shape[dim]) // (values.shape[dim] // blocks)).reshape([-1 if axis == dim else 1 for axis in range(values.ndim)]) for dim in (source, target)]
    chosen = jax.random.permutation(stream_key, blocks)[partner]
    strong = (owner == chosen) | (owner == (partner + blocks // 2) % blocks)
    return jnp.where(strong, factor * values, values)


def levels(rng, shape, cuts, smallest, high):
    def one(dim, blocks):
        draws = jax.random.uniform(jax.random.fold_in(jax.random.fold_in(rng, 6), dim), (blocks,), jnp.float32, smallest / len(cuts), high / len(cuts))
        return jnp.repeat(jnp.exp(draws), shape[dim] // blocks).reshape((-1,) + (1,) * (len(shape) - dim - 1))

    level = one(*cuts[0])
    for cut in cuts[1:]:
        level = level * one(*cut)
    return level


def profile(count, total, bound, lean):
    loads = [(1 << 20) // math.isqrt(grade ** lean) + 1 for grade in range(2, count + 1)]
    spare, given = total - bound - (count - 1), [1] * (count - 1)
    while spare > 0:
        movable = [i for i in range(count - 1) if given[i] < bound]
        pool, remaining = sum([loads[i] for i in movable]), spare
        for i in movable:
            extra = min(bound - given[i], max(1, remaining * loads[i] // pool), spare)
            given[i] = given[i] + extra
            spare = spare - extra
    return np.array([bound] + given)


def ragged_sizes(key, number_of, total, bound, skew):
    if number_of == 2:
        one = jax.random.randint(key, (), max(1, total - bound), min(bound, total - 1) + 1)
        return jnp.stack([one, total - one])
    sizes = jnp.asarray(profile(number_of, total, bound, skew), jnp.int32)
    twos = (number_of - 1) // 2
    giver, sink = sizes[1:1 + 2 * twos:2], sizes[2:2 + 2 * twos:2]
    slack = jnp.minimum(giver - 1, bound - sink)
    passed = jax.random.randint(jax.random.fold_in(key, 1), (twos,), 0, 1 << 20) % (slack + 1)
    sizes = sizes.at[1:1 + 2 * twos:2].set(giver - passed).at[2:2 + 2 * twos:2].set(sink + passed)
    return sizes[jax.random.permutation(jax.random.fold_in(key, 2), number_of)]


def bell_draw(rng, dims, scale, reach, cuts=(), kind=jnp.bfloat16):
    array = scale * jax.random.normal(rng, dims, jnp.float32)
    if cuts:
        array = array * levels(rng, dims, cuts, -0.22, 0.18)
    return jnp.clip(array, -reach, reach).astype(kind)


def gaussian_with(key, dims, scale, reach, pieces, heavy, kind=jnp.bfloat16):
    array = scale * jax.random.normal(key, dims, jnp.float32)
    if pieces:
        array = array * levels(key, dims, pieces, -0.22, 0.18)
    return jnp.clip(with_spikes(array, jax.random.fold_in(key, 3), *heavy), -reach, reach).astype(kind)


def setup_inputs(seed: int = 0) -> dict:
    key_of = jax.random.split(jax.random.key(seed), 6)
    return {
        "fields": draw_fields(jax.random.fold_in(key_of[5], 71), 0),
        "region_ids": jnp.searchsorted(jnp.cumsum(ragged_sizes(key_of[1], 2 * NLAT // WIN, NLAT, WIN, 0)), jnp.arange(NLAT), side="right").astype(jnp.int32),
        "w_qkv": draw_w_qkv(jax.random.fold_in(key_of[5], 71), 0),
        "w_proj": bell_draw(key_of[3], (C, C), C ** -0.5, 0.25, ((0, 32),)),
        "grad_output": gaussian_with(key_of[4], (NLAT, NLON, LEVELS, C), 1.0, 6.0, ((0, 4), (1, 8)), (1, 3, 8, 2.0)),
    }


EPSILON = 1e-05

def to_windows(grid, side):
    rows, cols, depth, width = grid.shape
    blocks = grid.reshape(rows // side, side, cols // side, side, depth, width)
    return blocks.transpose(0, 2, 1, 3, 4, 5).reshape(-1, side * side * depth, width)

def from_windows(windows, rows, cols, side):
    depth = windows.shape[1] // (side * side)
    width = windows.shape[2]
    blocks = windows.reshape(rows // side, cols // side, side, side, depth, width)
    return blocks.transpose(0, 2, 1, 3, 4, 5).reshape(rows, cols, depth, width)

def window_regions(region_ids, cols, depth, side):
    bands = region_ids.shape[0] // side
    spread = jnp.broadcast_to(region_ids.reshape(bands, 1, side, 1, 1), (bands, cols // side, side, side, depth))
    return spread.reshape(bands * (cols // side), side * side * depth)

def split_heads(qkv_window):
    count = qkv_window.shape[0]
    parts = qkv_window.reshape(count, 3, HEADS, HEAD).astype(jnp.float32)
    return (parts[:, 0], parts[:, 1], parts[:, 2])

def attention_probs(query, keys, region):
    scores = jnp.einsum('qhd,khd->hqk', query, keys, precision=lax.Precision.HIGHEST) * HEAD ** (-0.5)
    allowed = region[:, None] == region[None, :]
    scores = jnp.where(allowed[None], scores, -1e+30)
    peak = lax.optimization_barrier(jnp.max(scores, axis=-1, keepdims=True))
    weights = jnp.exp(scores - peak)
    return weights / lax.optimization_barrier(jnp.sum(weights, axis=-1, keepdims=True))

def forward_window(operands):
    qkv_window, region = operands
    query, keys, values = split_heads(qkv_window)
    probs = attention_probs(query, keys, region).astype(jnp.bfloat16).astype(jnp.float32)
    mixed = jnp.einsum('hqk,khd->qhd', probs, values, precision=lax.Precision.HIGHEST)
    return mixed.reshape(qkv_window.shape[0], C).astype(jnp.bfloat16)

def backward_window(operands):
    qkv_window, region, grad_window = operands
    count = qkv_window.shape[0]
    query, keys, values = split_heads(qkv_window)
    probs = attention_probs(query, keys, region)
    rounded = probs.astype(jnp.bfloat16).astype(jnp.float32)
    grad_heads = grad_window.reshape(count, HEADS, HEAD).astype(jnp.float32)
    grad_probs = jnp.einsum('qhd,khd->hqk', grad_heads, values, precision=lax.Precision.HIGHEST)
    grad_values = jnp.einsum('hqk,qhd->khd', rounded, grad_heads, precision=lax.Precision.HIGHEST)
    inner = lax.optimization_barrier(jnp.sum(grad_probs * probs, axis=-1, keepdims=True))
    grad_scores = (probs * (grad_probs - inner) * HEAD ** (-0.5)).astype(jnp.bfloat16).astype(jnp.float32)
    grad_query = jnp.einsum('hqk,khd->qhd', grad_scores, keys, precision=lax.Precision.HIGHEST)
    grad_keys = jnp.einsum('hqk,qhd->khd', grad_scores, query, precision=lax.Precision.HIGHEST)
    joined = jnp.stack([grad_query, grad_keys, grad_values], axis=1)
    return joined.reshape(count, 3 * C).astype(jnp.bfloat16)

def reference(fields, region_ids, w_qkv, w_proj, grad_output):
    half = WIN // 2
    count = NLAT * NLON * LEVELS
    factor = float(TOKENS) ** (-0.5)
    shifted = jnp.roll(fields, (-half, -half), axis=(0, 1))
    grad_shift = jnp.roll(grad_output, (-half, -half), axis=(0, 1))
    flat = shifted.reshape(count, C).astype(jnp.float32)
    centre = flat - lax.optimization_barrier(jnp.mean(flat, axis=-1, keepdims=True))
    inverse = lax.rsqrt(lax.optimization_barrier(jnp.mean(centre * centre, axis=-1, keepdims=True)) + EPSILON)
    normal = centre * inverse
    normed = normal.astype(jnp.bfloat16)
    qkv = jnp.dot(normed, w_qkv.T, preferred_element_type=jnp.float32).astype(jnp.bfloat16)
    regions = window_regions(region_ids, NLON, LEVELS, WIN)
    qkv_windows = to_windows(qkv.reshape(NLAT, NLON, LEVELS, 3 * C), WIN)
    attended_windows = lax.map(forward_window, (qkv_windows, regions))
    attended = from_windows(attended_windows, NLAT, NLON, WIN).reshape(count, C)
    branch = jnp.dot(attended, w_proj.T, preferred_element_type=jnp.float32).astype(jnp.bfloat16)
    branch_back = jnp.roll(branch.reshape(NLAT, NLON, LEVELS, C), (half, half), axis=(0, 1))
    block_out = (fields.astype(jnp.float32) + branch_back.astype(jnp.float32)).astype(jnp.bfloat16)
    grad_flat = grad_shift.reshape(count, C)
    grad_attended = jnp.dot(grad_flat, w_proj, preferred_element_type=jnp.float32).astype(jnp.bfloat16)
    grad_w_proj = jnp.dot(grad_flat.T, attended, preferred_element_type=jnp.float32) * factor
    grad_windows = to_windows(grad_attended.reshape(NLAT, NLON, LEVELS, C), WIN)
    grad_qkv_windows = lax.map(backward_window, (qkv_windows, regions, grad_windows))
    grad_qkv = from_windows(grad_qkv_windows, NLAT, NLON, WIN).reshape(count, 3 * C)
    grad_w_qkv = jnp.dot(grad_qkv.T, normed, preferred_element_type=jnp.float32) * factor
    grad_normed = jnp.dot(grad_qkv, w_qkv, preferred_element_type=jnp.float32)
    grad_pre = inverse * (grad_normed - lax.optimization_barrier(jnp.mean(grad_normed, axis=-1, keepdims=True)) - normal * lax.optimization_barrier(jnp.mean(grad_normed * normal, axis=-1, keepdims=True)))
    grad_pre = grad_pre.astype(jnp.bfloat16).reshape(NLAT, NLON, LEVELS, C)
    grad_back = jnp.roll(grad_pre, (half, half), axis=(0, 1))
    grad_fields = (grad_output.astype(jnp.float32) + grad_back.astype(jnp.float32)).astype(jnp.bfloat16)
    return (block_out, grad_fields, grad_w_qkv, grad_w_proj)
```

```python
import functools

import jax
import jax.numpy as jnp
from jax import lax
from jax.experimental import pallas as pl
from jax.experimental.pallas import tpu as pltpu
from jax.sharding import PartitionSpec as P

HEADS = 8
HEAD = 64
WIN = 12
HALF = WIN // 2
EPSILON = 1e-05
AXES = ("lon", "lat")
LANES = 128
SUB = 8


F32 = jnp.float32
BF16 = jnp.bfloat16


def nt(a, b):
    return lax.dot_general(a, b, (((1,), (1,)), ((), ())), preferred_element_type=F32)


def nn(a, b):
    return lax.dot_general(a, b, (((1,), (0,)), ((), ())), preferred_element_type=F32)


def sub_index(width):
    return lax.broadcasted_iota(jnp.int32, (SUB, width), 0)


def pick(own, strip):
    s = sub_index(own.shape[1])
    t0a, t1a, t2a, t0b, t1b, t2b = [own[8 * i : 8 * i + 8] for i in range(6)]
    ha, hb = strip[:8], strip[8:]
    mixed = jnp.where(
        s < 2,
        t2a,
        jnp.where(s < 4, pltpu.roll(t2b, 2, 0), jnp.where(s < 6, pltpu.roll(t0b, 6, 0), t0a)),
    )
    first = jnp.concatenate([t1a, t1b, mixed], axis=0)
    n1 = jnp.where(s < 2, ha, t2a)
    n2 = jnp.where(s < 2, hb, t2b)
    n3 = jnp.where((s >= 2) & (s < 6), ha, pltpu.roll(hb, 4, 0))
    second = jnp.concatenate([n1, n2, n3], axis=0)
    return first, second


def unpick(first, second):
    s = sub_index(first.shape[1])
    t1a, t1b, mixed = first[:8], first[8:16], first[16:]
    n1, n2, n3 = second[:8], second[8:16], second[16:]
    zero = jnp.zeros_like(mixed)
    t0a = jnp.where(s >= 6, mixed, zero)
    t0b = jnp.where(s >= 6, pltpu.roll(mixed, 2, 0), zero)
    t2a = jnp.where(s < 2, mixed, n1)
    t2b = jnp.where(s < 2, pltpu.roll(mixed, 6, 0), n2)
    ha = jnp.where(s < 2, n1, n3)
    hb = jnp.where(s < 2, n2, pltpu.roll(n3, 4, 0))
    own = jnp.concatenate([t0a, t1a, t2a, t0b, t1b, t2b], axis=0)
    return own, jnp.concatenate([ha, hb], axis=0)


def token_regions(region_ids, levels):
    lines = jnp.repeat(region_ids, levels)
    pairs = lines.reshape(-1, 2)
    s = jnp.arange(3 * SUB)
    inner = s % SUB
    line0 = jnp.where(s < 8, 0, jnp.where(s < 16, 1, jnp.where((inner < 2) | (inner >= 6), 0, 1)))
    line1 = jnp.where(s < 8, 0, jnp.where(s < 16, 1, jnp.where((inner >= 2) & (inner < 6), 0, 1)))
    a, b = pairs[:, :1], pairs[:, 1:]
    both = jnp.stack([jnp.where(line0 == 0, a, b), jnp.where(line1 == 0, a, b)])
    per_band = WIN * levels // 2
    bands = pairs.shape[0] // per_band
    return both.reshape(2, bands, per_band * 3 * SUB).transpose(1, 0, 2)


def assemble_kernel(own_ref, low_ref, east_ref, corner_ref, g_own, g_low, g_east, g_corner,
                    normed_ref, inv_ref, gs_ref, *, skip, upper):
    per_band = normed_ref.shape[2]

    def norm(block):
        centre = block - jnp.mean(block, axis=-1, keepdims=True)
        inverse = lax.rsqrt(jnp.mean(centre * centre, axis=-1, keepdims=True) + EPSILON)
        return (centre * inverse).astype(BF16), inverse

    def step(own, strip, g_o, g_s, at):
        band, place = at // per_band, at % per_band
        firsts = pick(own.astype(F32), strip.astype(F32))
        grads = pick(g_o.astype(F32), g_s.astype(F32))
        for j in range(2):
            normed, inverse = norm(firsts[j])
            normed_ref[band, j, place] = normed
            inv_ref[band, j, place] = jnp.broadcast_to(inverse, (3 * SUB, LANES))
            gs_ref[band, j, place] = grads[j].astype(BF16)

    @pl.loop(0, upper)
    def _(p):
        step(own_ref[p + skip], east_ref[p], g_own[p + skip], g_east[p], p)

    @pl.loop(0, skip)
    def _(p):
        step(low_ref[p], corner_ref[p], g_low[p], g_corner[p], p + upper)


def assemble(fields, low, east, corner, grads, g_low, g_east, g_corner):
    pairs, _, width = fields.shape
    skip = low.shape[0]
    upper = east.shape[0]
    per_band = 2 * skip
    bands = (upper + skip) // per_band
    shape = (bands, 2, per_band, 3 * SUB)
    return pl.pallas_call(
        functools.partial(assemble_kernel, skip=skip, upper=upper),
        out_shape=(
            jax.ShapeDtypeStruct(shape + (width,), BF16),
            jax.ShapeDtypeStruct(shape + (LANES,), F32),
            jax.ShapeDtypeStruct(shape + (width,), BF16),
        ),
        name="assemble",
    )(fields, low, east, corner, grads, g_low, g_east, g_corner)


def attention_kernel(normed_ref, gs_ref, reg_col_ref, reg_row_ref, w_ref, wp_ref,
                     att_ref, gqkv_ref, gw_ref, gp_ref, gw_acc, gp_acc):
    window = pl.program_id(1)
    scale = HEAD ** (-0.5)
    normed = normed_ref[window]
    grads = gs_ref[window]
    count = normed.shape[0]
    weights = w_ref[...].reshape(3 * LANES, w_ref.shape[2])
    qkv = nt(normed, weights).astype(BF16)
    query, keys, values = [qkv[:, LANES * i : LANES * (i + 1)] for i in range(3)]
    query = query * jnp.asarray(scale, BF16)
    grad_att = nn(grads, wp_ref[...]).astype(BF16)
    keys_t = keys.astype(F32).T.astype(BF16) * jnp.asarray(scale, BF16)
    values_t = values.astype(F32).T.astype(BF16)
    allowed = reg_col_ref[window] == reg_row_ref[window]
    lane = lax.broadcasted_iota(jnp.int32, (count, LANES), 1)
    att_t, grad_q_t = [], []
    grad_k = grad_v = None
    for h in range(LANES // HEAD):
        mine = (lane >= h * HEAD) & (lane < (h + 1) * HEAD)
        zero = jnp.zeros((), BF16)
        rows = slice(h * HEAD, (h + 1) * HEAD)
        scores = nt(jnp.where(mine, keys, zero), query)
        scores = jnp.where(allowed, scores, -1e30)
        peak = jnp.max(scores, axis=0, keepdims=True)
        expo = jnp.exp(scores - peak)
        probs = expo * (1.0 / jnp.sum(expo, axis=0, keepdims=True))
        rounded = probs.astype(BF16)
        grad_probs = nt(jnp.where(mine, values, zero), grad_att)
        inner = jnp.sum(grad_probs * probs, axis=0, keepdims=True)
        grad_scores = (probs * (grad_probs - inner)).astype(BF16)
        att_t.append(nn(values_t[rows], rounded))
        grad_q_t.append(nn(keys_t[rows], grad_scores))
        part_v = nn(rounded, jnp.where(mine, grad_att, zero))
        part_k = nn(grad_scores, jnp.where(mine, query, zero))
        grad_v = part_v if grad_v is None else grad_v + part_v
        grad_k = part_k if grad_k is None else grad_k + part_k
    att_t = jnp.concatenate(att_t, axis=0)
    grad_q_t = jnp.concatenate(grad_q_t, axis=0)
    att_ref[0] = att_t.T.astype(BF16)
    gqkv_ref[0, 0] = grad_q_t.T.astype(BF16)
    gqkv_ref[0, 1] = grad_k.astype(BF16)
    gqkv_ref[0, 2] = grad_v.astype(BF16)
    grad_w = (
        nn(grad_q_t.astype(BF16), normed),
        nn(grad_k.T.astype(BF16), normed),
        nn(grad_v.T.astype(BF16), normed),
    )
    grad_p = nn(att_t.astype(BF16), grads)

    @pl.when(window == 0)
    def _():
        for i in range(3):
            gw_acc[i] = grad_w[i]
        gp_acc[...] = grad_p

    @pl.when(window > 0)
    def _():
        for i in range(3):
            gw_acc[i] += grad_w[i]
        gp_acc[...] += grad_p

    @pl.when(window == pl.num_programs(1) - 1)
    def _():
        gw_ref[...] = gw_acc[...]
        gp_ref[...] = gp_acc[...]


def attention(normed, gs, reg_col, reg_row, w_qkv, w_proj):
    windows, count, width = normed.shape
    groups = width // LANES
    whole = lambda *shape: pl.BlockSpec(shape, lambda p, w: (0,) * len(shape))
    return pl.pallas_call(
        attention_kernel,
        grid=(groups, windows),
        in_specs=[
            whole(windows, count, width),
            whole(windows, count, width),
            whole(windows, count, 1),
            whole(windows, 1, count),
            pl.BlockSpec((3, LANES, width), lambda p, w: (0, p, 0)),
            pl.BlockSpec((width, LANES), lambda p, w: (0, p)),
        ],
        out_specs=[
            pl.BlockSpec((1, count, LANES), lambda p, w: (w, 0, p)),
            pl.BlockSpec((1, 3, count, LANES), lambda p, w: (w, 0, 0, p)),
            pl.BlockSpec((3, LANES, width), lambda p, w: (0, p, 0)),
            pl.BlockSpec((LANES, width), lambda p, w: (p, 0)),
        ],
        out_shape=(
            jax.ShapeDtypeStruct((windows, count, width), BF16),
            jax.ShapeDtypeStruct((windows, 3, count, width), BF16),
            jax.ShapeDtypeStruct((3, width, width), F32),
            jax.ShapeDtypeStruct((width, width), F32),
        ),
        scratch_shapes=[pltpu.VMEM((3, LANES, width), F32), pltpu.VMEM((LANES, width), F32)],
        name="attention",
    )(normed, gs, reg_col, reg_row, w_qkv, w_proj)


def finish_kernel(att_ref, gqkv_ref, normed_ref, inv_ref, w_ref, wp_ref, fields_ref, grads_ref,
                  out_ref, gout_ref, low_ref, east_ref, corner_ref, g_low, g_east, g_corner,
                  branch_scr, pre_scr):
    band = pl.program_id(0)
    skip = low_ref.shape[0]
    per_band = 2 * skip
    width = wp_ref.shape[0]
    for j in range(2):
        branch = nt(att_ref[0, j], wp_ref[...])
        branch_scr[j] = branch.astype(BF16).astype(F32).reshape(per_band, 3 * SUB, width)
        grad_normed = nn(gqkv_ref[0, j, 0], w_ref[0])
        grad_normed += nn(gqkv_ref[0, j, 1], w_ref[1])
        grad_normed += nn(gqkv_ref[0, j, 2], w_ref[2])
        normal = normed_ref[0, j].astype(F32)
        mean = jnp.mean(grad_normed, axis=-1, keepdims=True)
        along = jnp.mean(grad_normed * normal, axis=-1, keepdims=True)
        pre = inv_ref[0, j][:, :1] * (grad_normed - mean - normal * along)
        pre_scr[j] = pre.astype(BF16).astype(F32).reshape(per_band, 3 * SUB, width)

    def own(p, at):
        add, strip = unpick(branch_scr[0, p], branch_scr[1, p])
        out_ref[at] = (fields_ref[at].astype(F32) + add).astype(BF16)
        east_ref[at - skip] = strip.astype(BF16)
        add, strip = unpick(pre_scr[0, p], pre_scr[1, p])
        gout_ref[at] = (grads_ref[at].astype(F32) + add).astype(BF16)
        g_east[at - skip] = strip.astype(BF16)

    def away(p, at):
        add, strip = unpick(branch_scr[0, p], branch_scr[1, p])
        low_ref[at] = add.astype(BF16)
        corner_ref[at] = strip.astype(BF16)
        add, strip = unpick(pre_scr[0, p], pre_scr[1, p])
        g_low[at] = add.astype(BF16)
        g_corner[at] = strip.astype(BF16)

    last = band == pl.num_programs(0) - 1

    @pl.loop(0, skip)
    def _(p):
        own(p, p + skip + band * per_band)

    @pl.when(jnp.logical_not(last))
    def _():
        @pl.loop(skip, per_band)
        def _(p):
            own(p, p + skip + band * per_band)

    @pl.when(last)
    def _():
        @pl.loop(skip, per_band)
        def _(p):
            away(p, p - skip)


def finish(att, gqkv, normed, inv, w_qkv, w_proj, fields, grads):
    bands, _, count, width = att.shape
    pairs = fields.shape[0]
    per_band = count // (3 * SUB)
    skip = per_band // 2
    upper = pairs - skip
    whole = lambda *shape: pl.BlockSpec(shape, lambda b: (0,) * len(shape))
    banded = lambda *shape: pl.BlockSpec((1,) + shape, lambda b: (b,) + (0,) * len(shape))
    outs = [(pairs, 48, width)] * 2 + [(skip, 48, width), (upper, 16, width), (skip, 16, width)] * 2
    return pl.pallas_call(
        finish_kernel,
        grid=(bands,),
        in_specs=[
            banded(2, count, width),
            banded(2, 3, count, width),
            banded(2, count, width),
            banded(2, count, LANES),
            whole(3, width, width),
            whole(width, width),
            whole(pairs, 48, width),
            whole(pairs, 48, width),
        ],
        out_specs=[whole(*shape) for shape in outs],
        out_shape=tuple(jax.ShapeDtypeStruct(shape, BF16) for shape in outs),
        scratch_shapes=[
            pltpu.VMEM((2, per_band, 3 * SUB, width), F32),
            pltpu.VMEM((2, per_band, 3 * SUB, width), F32),
        ],
        name="finish",
    )(att, gqkv, normed, inv, w_qkv, w_proj, fields, grads)


def edge_kernel(f_ref, o_ref, r_ref, g_ref, q_ref, gr_ref, out_ref, gout_ref):
    shape = f_ref.shape
    s = lax.broadcasted_iota(jnp.int32, shape, 1)
    for f, o, r, out in ((f_ref, o_ref, r_ref, out_ref), (g_ref, q_ref, gr_ref, gout_ref)):
        total = f[...].astype(F32) + r[...].astype(F32)
        out[...] = jnp.where(s < HALF, total, o[...].astype(F32)).astype(BF16)


def edge(fields, out, back, grads, gout, g_back, skip):
    lines, cols, width = fields.shape
    n = back.shape[0] // skip
    at = pl.BlockSpec((skip, SUB, width), lambda i: (i + 1, 0, 0))
    strip = pl.BlockSpec((skip, SUB, width), lambda i: (i, 0, 0))
    return pl.pallas_call(
        edge_kernel,
        grid=(n,),
        in_specs=[at, at, strip, at, at, strip],
        out_specs=[at, at],
        out_shape=(jax.ShapeDtypeStruct(out.shape, BF16),) * 2,
        input_output_aliases={1: 0, 4: 1},
        name="edge",
    )(fields, out, back, grads, gout, g_back)


def rim_kernel(f_ref, low_ref, c_ref, g_ref, g_low, gc_ref, out_any, gout_any, out_ref, gout_ref):
    for f, low, c, out in ((f_ref, low_ref, c_ref, out_ref), (g_ref, g_low, gc_ref, gout_ref)):
        back = low[...].astype(F32)
        s = lax.broadcasted_iota(jnp.int32, c.shape, 1)
        head = jnp.where(s < HALF, c[...].astype(F32), back[:, :SUB])
        back = jnp.concatenate([head, back[:, SUB:]], axis=1)
        out[...] = (f[...].astype(F32) + back).astype(BF16)


def rim(fields, low, corner, grads, g_low, g_corner, out, gout):
    skip = low.shape[0]
    _, cols, width = fields.shape
    at = pl.BlockSpec((skip, cols, width), lambda i: (0, 0, 0))
    strip = pl.BlockSpec((skip, SUB, width), lambda i: (0, 0, 0))
    anyw = pl.BlockSpec(memory_space=pl.ANY)
    return pl.pallas_call(
        rim_kernel,
        grid=(1,),
        in_specs=[at, at, strip, at, at, strip, anyw, anyw],
        out_specs=[at, at],
        out_shape=(jax.ShapeDtypeStruct(out.shape, BF16),) * 2,
        input_output_aliases={6: 0, 7: 1},
        name="rim",
    )(fields, low, corner, grads, g_low, g_corner, out, gout)


def linear(lon, lat, lats):
    return lon * lats + lat


def shift_by(block, step_lon, step_lat):
    lons, lats = lax.axis_size("lon"), lax.axis_size("lat")
    route = [
        (linear((i + step_lon) % lons, (j + step_lat) % lats, lats), linear(i, j, lats))
        for i in range(lons)
        for j in range(lats)
    ]
    return lax.ppermute(block, AXES, route)


def bit_order():
    lons, lats = lax.axis_size("lon"), lax.axis_size("lat")
    lat_bits = [1 << i for i in range(lats.bit_length() - 1)]
    lon_bits = [lats << i for i in range(lons.bit_length() - 1)]
    assert lats == 1 << len(lat_bits) and lons == 1 << len(lon_bits)
    return lat_bits, lon_bits


def swap(block, bit):
    total = lax.axis_size("lon") * lax.axis_size("lat")
    return lax.ppermute(block, AXES, [(i, i ^ bit) for i in range(total)])


def gather_rows(block):
    lat_bits, lon_bits = bit_order()
    order = lat_bits[::-1] + lon_bits[1:] + lon_bits[:1]
    bits = sorted(order)[::-1]
    place = lax.axis_index(AXES)
    held = block.reshape((1,) * len(bits) + block.shape)
    for bit in order:
        axis = bits.index(bit)
        other = swap(held, bit)
        high = (place & bit) != 0
        held = jnp.concatenate(
            [jnp.where(high, other, held), jnp.where(high, held, other)], axis=axis
        )
    return held.reshape((-1,) + block.shape[1:])


def scatter_sum(blocks):
    lat_bits, lon_bits = bit_order()
    order = lon_bits[:1] + lon_bits[1:][::-1] + lat_bits
    bits = sorted(order)[::-1]
    place = lax.axis_index(AXES)
    held = blocks.reshape((2,) * len(bits) + blocks.shape[1:])
    for bit in order:
        axis = bits.index(bit)
        mine = jnp.where((place & bit) != 0, 1, 0)
        keep = lax.dynamic_index_in_dim(held, mine, axis, keepdims=True)
        send = lax.dynamic_index_in_dim(held, 1 - mine, axis, keepdims=True).astype(BF16)
        held = keep + swap(send, bit).astype(F32)
    return held.reshape(blocks.shape[1:])


def lines_of(grid):
    rows, cols, levels, width = grid.shape
    return grid.transpose(0, 2, 1, 3).reshape(rows * levels, cols, width)


def grid_of(lines, levels):
    count, cols, width = lines.shape
    return lines.reshape(count // levels, levels, cols, width).transpose(0, 2, 1, 3)


def paired(lines):
    count, cols, width = lines.shape
    return lines.reshape(count // 2, 2 * cols, width)


def unpaired(pairs):
    count, cols, width = pairs.shape
    return pairs.reshape(count * 2, cols // 2, width)


def shards(fields, region_ids, w_qkv, w_proj, grad_output):
    rows, cols, levels, width = fields.shape
    skip = HALF * levels
    devices = lax.axis_size("lon") * lax.axis_size("lat")
    factor = float(rows * cols * levels * devices) ** (-0.5)
    w_all = gather_rows(w_qkv)
    p_all = gather_rows(w_proj)
    f_lines, g_lines = lines_of(fields), lines_of(grad_output)
    east, g_east = [shift_by(x[skip:, :SUB], 1, 0) for x in (f_lines, g_lines)]
    low, g_low = [shift_by(x[:skip], 0, 1) for x in (f_lines, g_lines)]
    corner, g_corner = [shift_by(x[:skip, :SUB], 1, 1) for x in (f_lines, g_lines)]
    normed, inv, gs = assemble(
        *[paired(x) for x in (f_lines, low, east, corner, g_lines, g_low, g_east, g_corner)]
    )
    bands = normed.shape[0]
    count = WIN * WIN * levels
    regions = token_regions(region_ids, levels).reshape(2 * bands, count)
    flat = lambda x: x.reshape(2 * bands, count, x.shape[-1])
    w3 = w_all.reshape(3, width, width)
    att, gqkv, grad_w, grad_p = attention(
        flat(normed), flat(gs), regions[:, :, None], regions[:, None, :], w3, p_all
    )
    blocks = jnp.concatenate(
        [
            grad_w.reshape(devices, -1, width),
            grad_p.T.reshape(devices, -1, width),
        ],
        axis=1,
    )
    out, gout, r_low, r_east, r_corner, gr_low, gr_east, gr_corner = finish(
        att.reshape(bands, 2, count, width),
        gqkv.reshape(bands, 2, 3, count, width),
        normed.reshape(bands, 2, count, width),
        inv.reshape(bands, 2, count, LANES),
        w3,
        p_all,
        paired(f_lines),
        paired(g_lines),
    )
    own = scatter_sum(blocks) * factor
    r_low, gr_low = [shift_by(unpaired(x), 0, -1) for x in (r_low, gr_low)]
    r_east, gr_east = [shift_by(unpaired(x), -1, 0) for x in (r_east, gr_east)]
    r_corner, gr_corner = [shift_by(unpaired(x), -1, -1) for x in (r_corner, gr_corner)]
    out, gout = edge(f_lines, unpaired(out), r_east, g_lines, unpaired(gout), gr_east, skip)
    out, gout = rim(f_lines, r_low, r_corner, g_lines, gr_low, gr_corner, out, gout)
    share = w_qkv.shape[0]
    return (grid_of(out, levels), grid_of(gout, levels), own[:share], own[share:])


def solution(mesh):
    return jax.shard_map(
        shards,
        mesh=mesh,
        in_specs=(
            P("lat", "lon", None, None),
            P("lat"),
            P(AXES, None),
            P(AXES, None),
            P("lat", "lon", None, None),
        ),
        out_specs=(
            P("lat", "lon", None, None),
            P("lat", "lon", None, None),
            P(AXES, None),
            P(AXES, None),
        ),
        check_vma=False,
    )
```

```python
import functools

import jax
import jax.numpy as jnp
from jax import lax
from jax.experimental import pallas as pl
from jax.experimental.pallas import tpu as pltpu
from jax.sharding import PartitionSpec as P


HEAD = 64
WIN = 12
HALF = WIN // 2
EPSILON = 1e-05
AXES = ("lon", "lat")
LANES = 128
SUB = 8


F32 = jnp.float32
BF16 = jnp.bfloat16


def nt(a, b):
    return lax.dot_general(a, b, (((1,), (1,)), ((), ())), preferred_element_type=F32)


def nn(a, b):
    return lax.dot_general(a, b, (((1,), (0,)), ((), ())), preferred_element_type=F32)


def sub_index(width):
    return lax.broadcasted_iota(jnp.int32, (SUB, width), 0)


def pick_first(own):
    s = sub_index(own.shape[1])
    t0a, t1a, t2a, t0b, t1b, t2b = [own[8 * i : 8 * i + 8] for i in range(6)]
    mixed = jnp.where(
        s < 2,
        t2a,
        jnp.where(s < 4, pltpu.roll(t2b, 2, 0), jnp.where(s < 6, pltpu.roll(t0b, 6, 0), t0a)),
    )
    return jnp.concatenate([t1a, t1b, mixed], axis=0)


def pick_second(own, strip):
    s = sub_index(own.shape[1])
    t2a, t2b = own[16:24], own[40:48]
    ha, hb = strip[:8], strip[8:]
    n1 = jnp.where(s < 2, ha, t2a)
    n2 = jnp.where(s < 2, hb, t2b)
    n3 = jnp.where((s >= 2) & (s < 6), ha, pltpu.roll(hb, 4, 0))
    return jnp.concatenate([n1, n2, n3], axis=0)


def unpick(first, second):
    s = sub_index(first.shape[1])
    t1a, t1b, mixed = first[:8], first[8:16], first[16:]
    n1, n2, n3 = second[:8], second[8:16], second[16:]
    zero = jnp.zeros_like(mixed)
    t0a = jnp.where(s >= 6, mixed, zero)
    t0b = jnp.where(s >= 6, pltpu.roll(mixed, 2, 0), zero)
    t2a = jnp.where(s < 2, mixed, n1)
    t2b = jnp.where(s < 2, pltpu.roll(mixed, 6, 0), n2)
    ha = jnp.where(s < 2, n1, n3)
    hb = jnp.where(s < 2, n2, pltpu.roll(n3, 4, 0))
    own = jnp.concatenate([t0a, t1a, t2a, t0b, t1b, t2b], axis=0)
    return own, jnp.concatenate([ha, hb], axis=0)


def token_regions(region_ids, levels):
    lines = jnp.repeat(region_ids, levels)
    pairs = lines.reshape(-1, 2)
    s = jnp.arange(3 * SUB)
    inner = s % SUB
    line0 = jnp.where(s < 8, 0, jnp.where(s < 16, 1, jnp.where((inner < 2) | (inner >= 6), 0, 1)))
    line1 = jnp.where(s < 8, 0, jnp.where(s < 16, 1, jnp.where((inner >= 2) & (inner < 6), 0, 1)))
    a, b = pairs[:, :1], pairs[:, 1:]
    both = jnp.stack([jnp.where(line0 == 0, a, b), jnp.where(line1 == 0, a, b)])
    per_band = WIN * levels // 2
    bands = pairs.shape[0] // per_band
    return both.reshape(2, bands, per_band * 3 * SUB).transpose(1, 0, 2)


def norm(block):
    centre = block - jnp.mean(block, axis=-1, keepdims=True)
    inverse = lax.rsqrt(jnp.mean(centre * centre, axis=-1, keepdims=True) + EPSILON)
    return (centre * inverse).astype(BF16), inverse


def put(at, p, block, grads, normed_ref, inv_ref, gs_ref):
    normed, inverse = norm(block)
    normed_ref[at, p] = normed
    inv_ref[at, p] = jnp.broadcast_to(inverse, (3 * SUB, LANES))
    gs_ref[at, p] = grads.astype(BF16)


def assemble_own_kernel(f_ref, g_ref, *outs):
    @pl.loop(0, f_ref.shape[0], unroll=3)
    def _(p):
        put(0, p, pick_first(f_ref[p].astype(F32)), pick_first(g_ref[p].astype(F32)), *outs)


def assemble_east_kernel(f_ref, g_ref, east_ref, *outs):
    @pl.loop(0, f_ref.shape[0], unroll=3)
    def _(p):
        put(
            0,
            p,
            pick_second(f_ref[p].astype(F32), east_ref[0, p].astype(F32)),
            pick_second(g_ref[p].astype(F32), east_ref[1, p].astype(F32)),
            *outs,
        )


def assemble_low_kernel(f_ref, g_ref, east_ref, low_ref, corner_ref, *outs):
    def both(p, f, g, fs, gs):
        f, g = f.astype(F32), g.astype(F32)
        put(0, p, pick_first(f), pick_first(g), *outs)
        put(1, p, pick_second(f, fs.astype(F32)), pick_second(g, gs.astype(F32)), *outs)

    @pl.when(pl.program_id(0) == 0)
    def _():
        @pl.loop(0, f_ref.shape[0], unroll=3)
        def _(p):
            both(p, f_ref[p], g_ref[p], east_ref[0, p], east_ref[1, p])

    @pl.when(pl.program_id(0) == 1)
    def _():
        @pl.loop(0, f_ref.shape[0], unroll=3)
        def _(p):
            both(p, low_ref[0, p], low_ref[1, p], corner_ref[0, p], corner_ref[1, p])


def assembled(kernel, windows, skip, width, specs, args):
    shape = (windows, 2 * skip, 3 * SUB)
    out = lambda w: pl.BlockSpec((windows, skip, 3 * SUB, w), lambda s: (0, s, 0, 0))
    outs = pl.pallas_call(
        kernel,
        grid=(2,),
        in_specs=specs,
        out_specs=[out(width), out(LANES), out(width)],
        out_shape=(
            jax.ShapeDtypeStruct(shape + (width,), BF16),
            jax.ShapeDtypeStruct(shape + (LANES,), F32),
            jax.ShapeDtypeStruct(shape + (width,), BF16),
        ),
        cost_estimate=pl.CostEstimate(
            flops=windows * skip * 3 * SUB * width * 100, transcendentals=0,
            bytes_accessed=windows * skip * 3 * SUB * width * 16),
    )(*args)
    count = 2 * skip * 3 * SUB
    return [x.reshape(windows, count, x.shape[-1]) for x in outs]


def assemble_own(fields, grads, skip):
    width = fields.shape[2]
    own = pl.BlockSpec((skip, 48, width), lambda s: (s + 1, 0, 0))
    return assembled(assemble_own_kernel, 1, skip, width, [own, own], (fields, grads))


def assemble_east(fields, grads, east, skip):
    width = fields.shape[2]
    own = pl.BlockSpec((skip, 48, width), lambda s: (s + 1, 0, 0))
    strip = pl.BlockSpec((2, skip, 16, width), lambda s: (0, s, 0, 0))
    return assembled(assemble_east_kernel, 1, skip, width, [own, own, strip], (fields, grads, east))


def assemble_low(fields, grads, east, low, corner, skip):
    width = fields.shape[2]
    last = fields.shape[0] // skip - 1
    own = pl.BlockSpec((skip, 48, width), lambda s: (last, 0, 0))
    strip = pl.BlockSpec((2, skip, 16, width), lambda s: (0, last - 1, 0, 0))
    below = pl.BlockSpec((2, skip, 48, width), lambda s: (0, 0, 0, 0))
    diagonal = pl.BlockSpec((2, skip, 16, width), lambda s: (0, 0, 0, 0))
    return assembled(
        assemble_low_kernel, 2, skip, width, [own, own, strip, below, diagonal],
        (fields, grads, east, low, corner),
    )


def attention_kernel(*refs, carried, last):
    normed_ref, gs_ref, reg_col_ref, reg_row_ref, w_ref, wp_ref = refs[:6]
    refs = refs[6:]
    if carried:
        gw_in, gp_in = refs[:2]
        refs = refs[2:]
    att_ref, gqkv_ref, gw_ref, gp_ref = refs[:4]
    gw_acc, gp_acc = refs[4:] if last else (gw_ref, gp_ref)
    window = pl.program_id(1)
    scale = HEAD ** (-0.5)
    normed = normed_ref[window]
    grads = gs_ref[window]
    count = normed.shape[0]
    weights = w_ref[...].reshape(3 * LANES, w_ref.shape[2])
    qkv = nt(normed, weights).astype(BF16)
    query, keys, values = [qkv[:, LANES * i : LANES * (i + 1)] for i in range(3)]
    query = query * jnp.asarray(scale, BF16)
    grad_att = nn(grads, wp_ref[...]).astype(BF16)
    keys_t = keys.astype(F32).T.astype(BF16) * jnp.asarray(scale, BF16)
    values_t = values.astype(F32).T.astype(BF16)
    allowed = reg_col_ref[window] == reg_row_ref[window]
    lane = lax.broadcasted_iota(jnp.int32, (count, LANES), 1)
    att_t, grad_q_t = [], []
    grad_k = grad_v = None
    for h in range(LANES // HEAD):
        mine = (lane >= h * HEAD) & (lane < (h + 1) * HEAD)
        zero = jnp.zeros((), BF16)
        rows = slice(h * HEAD, (h + 1) * HEAD)
        scores = nt(jnp.where(mine, keys, zero), query)
        scores = jnp.where(allowed, scores, -1e30)
        peak = jnp.max(scores, axis=0, keepdims=True)
        expo = jnp.exp(scores - peak)
        probs = expo * (1.0 / jnp.sum(expo, axis=0, keepdims=True))
        rounded = probs.astype(BF16)
        grad_probs = nt(jnp.where(mine, values, zero), grad_att)
        inner = jnp.sum(grad_probs * probs, axis=0, keepdims=True)
        grad_scores = (probs * (grad_probs - inner)).astype(BF16)
        att_t.append(nn(values_t[rows], rounded))
        grad_q_t.append(nn(keys_t[rows], grad_scores))
        part_v = nn(rounded, jnp.where(mine, grad_att, zero))
        part_k = nn(grad_scores, jnp.where(mine, query, zero))
        grad_v = part_v if grad_v is None else grad_v + part_v
        grad_k = part_k if grad_k is None else grad_k + part_k
    att_t = jnp.concatenate(att_t, axis=0)
    grad_q_t = jnp.concatenate(grad_q_t, axis=0)
    att_ref[0] = att_t.T.astype(BF16)
    gqkv_ref[0, 0] = grad_q_t.T.astype(BF16)
    gqkv_ref[0, 1] = grad_k.astype(BF16)
    gqkv_ref[0, 2] = grad_v.astype(BF16)
    grad_w = (
        nn(grad_q_t.astype(BF16), normed),
        nn(grad_k.T.astype(BF16), normed),
        nn(grad_v.T.astype(BF16), normed),
    )
    grad_p = nn(att_t.astype(BF16), grads)

    @pl.when(window == 0)
    def _():
        for i in range(3):
            gw_acc[i] = grad_w[i] + gw_in[i] if carried else grad_w[i]
        gp_acc[...] = grad_p + gp_in[...] if carried else grad_p

    @pl.when(window > 0)
    def _():
        for i in range(3):
            gw_acc[i] += grad_w[i]
        gp_acc[...] += grad_p

    if last:

        @pl.when(window == pl.num_programs(1) - 1)
        def _():
            gw_ref[...] = gw_acc[...].astype(BF16)
            gp_ref[...] = gp_acc[...].T.astype(BF16)


def attention(normed, gs, regions, w_qkv, w_proj, carry=(), last=False):
    windows, count, width = normed.shape
    groups = width // LANES
    whole = lambda *shape: pl.BlockSpec(shape, lambda p, w: (0,) * len(shape))
    rows3 = pl.BlockSpec((3, LANES, width), lambda p, w: (0, p, 0))
    rows1 = pl.BlockSpec((LANES, width), lambda p, w: (p, 0))
    cols1 = pl.BlockSpec((width, LANES), lambda p, w: (0, p))
    kind = BF16 if last else F32
    scratch = [pltpu.VMEM((3, LANES, width), F32), pltpu.VMEM((LANES, width), F32)]
    return pl.pallas_call(
        functools.partial(attention_kernel, carried=bool(carry), last=last),
        grid=(groups, windows),
        in_specs=[
            whole(windows, count, width),
            whole(windows, count, width),
            whole(windows, count, 1),
            whole(windows, 1, count),
            rows3,
            cols1,
        ]
        + ([rows3, rows1] if carry else []),
        out_specs=[
            pl.BlockSpec((1, count, LANES), lambda p, w: (w, 0, p)),
            pl.BlockSpec((1, 3, count, LANES), lambda p, w: (w, 0, 0, p)),
            rows3,
            cols1 if last else rows1,
        ],
        out_shape=(
            jax.ShapeDtypeStruct((windows, count, width), BF16),
            jax.ShapeDtypeStruct((windows, 3, count, width), BF16),
            jax.ShapeDtypeStruct((3, width, width), kind),
            jax.ShapeDtypeStruct((width, width), kind),
        ),
        scratch_shapes=scratch if last else [],
        cost_estimate=pl.CostEstimate(
            flops=windows * count * width * (16 * width + 12 * count), transcendentals=0,
            bytes_accessed=windows * count * width * 12),
    )(normed, gs, regions[:, :, None], regions[:, None, :], w_qkv, w_proj, *carry)


def finish_kernel(*refs, low):
    ins = refs[:8]
    w_ref, wp_ref, fields_ref, grads_ref = refs[8:12]
    branch_scr, pre_scr = refs[-2:]
    outs = refs[12:-2] if low else refs[14:-2]
    out_ref, gout_ref, east_ref = outs[:3]
    n = fields_ref.shape[0]
    width = wp_ref.shape[0]
    for j in range(2):
        att, gqkv, normed, inv = ins[4 * j : 4 * j + 4]
        branch = nt(att[0], wp_ref[...])
        branch_scr[j] = branch.astype(BF16).astype(F32).reshape(n, 3 * SUB, width)
        grad_normed = nn(gqkv[0, 0], w_ref[0]) + nn(gqkv[0, 1], w_ref[1]) + nn(gqkv[0, 2], w_ref[2])
        normal = normed[0].astype(F32)
        mean = jnp.mean(grad_normed, axis=-1, keepdims=True)
        along = jnp.mean(grad_normed * normal, axis=-1, keepdims=True)
        pre = inv[0][:, :1] * (grad_normed - mean - normal * along)
        pre_scr[j] = pre.astype(BF16).astype(F32).reshape(n, 3 * SUB, width)

    def own():
        @pl.loop(0, n, unroll=3)
        def _(p):
            add, strip = unpick(branch_scr[0, p], branch_scr[1, p])
            out_ref[p] = (fields_ref[p].astype(F32) + add).astype(BF16)
            east_ref[0, p] = strip.astype(BF16)
            add, strip = unpick(pre_scr[0, p], pre_scr[1, p])
            gout_ref[p] = (grads_ref[p].astype(F32) + add).astype(BF16)
            east_ref[1, p] = strip.astype(BF16)

    if not low:
        own()
        return
    low_ref, corner_ref = outs[3:]
    pl.when(pl.program_id(0) == 0)(own)

    @pl.when(pl.program_id(0) == 1)
    def _():
        @pl.loop(0, n, unroll=3)
        def _(p):
            for i, scr in enumerate((branch_scr, pre_scr)):
                add, strip = unpick(scr[0, p], scr[1, p])
                low_ref[i, p] = add.astype(BF16)
                corner_ref[i, p] = strip.astype(BF16)


def finish(sets, places, w_qkv, w_proj, fields, grads, skip, low, into=()):
    pairs, _, width = fields.shape
    last = pairs // skip - 1
    part = skip * 3 * SUB
    own = pl.BlockSpec((skip, 48, width), (lambda s: (last, 0, 0)) if low else (lambda s: (s + 1, 0, 0)))
    whole = lambda *shape: pl.BlockSpec(shape, lambda s: (0,) * len(shape))
    specs, args = [], []
    for (att, gqkv, normed, inv), at in zip(sets, places):
        specs += [
            pl.BlockSpec((1, part, width), lambda s, at=at: (at, s, 0)),
            pl.BlockSpec((1, 3, part, width), lambda s, at=at: (at, 0, s, 0)),
            pl.BlockSpec((1, part, width), lambda s, at=at: (at, s, 0)),
            pl.BlockSpec((1, part, LANES), lambda s, at=at: (at, s, 0)),
        ]
        args += [att, gqkv, normed, inv]
    specs += [whole(3, width, width), whole(width, width), own, own]
    args += [w_qkv, w_proj, fields, grads]
    alias = {}
    if not low:
        alias = {len(args): 0, len(args) + 1: 1}
        specs += [pl.BlockSpec(memory_space=pl.ANY)] * 2
        args += list(into)
    shapes = [(pairs, 48, width)] * 2 + [(2, skip if low else 2 * skip, 16, width)]
    outs = [own, own]
    if low:
        shapes += [(2, skip, 48, width), (2, skip, 16, width)]
        outs += [whole(*shape) for shape in shapes[2:]]
    else:
        outs += [pl.BlockSpec((2, skip, 16, width), lambda s: (0, s, 0, 0))]
    return pl.pallas_call(
        functools.partial(finish_kernel, low=low),
        grid=(2,),
        in_specs=specs,
        out_specs=outs,
        out_shape=tuple(jax.ShapeDtypeStruct(shape, BF16) for shape in shapes),
        scratch_shapes=[pltpu.VMEM((2, skip, 3 * SUB, width), F32)] * 2,
        input_output_aliases=alias,
        cost_estimate=pl.CostEstimate(
            flops=4 * part * 8 * width * width, transcendentals=0, bytes_accessed=8 * part * width * 16),
        name="finish_low" if low else "finish_top",
    )(*args)


def edge_kernel(f_ref, o_ref, r_ref, g_ref, q_ref, out_ref, gout_ref):
    s = lax.broadcasted_iota(jnp.int32, f_ref.shape, 1)
    for i, (f, o, out) in enumerate(((f_ref, o_ref, out_ref), (g_ref, q_ref, gout_ref))):
        total = f[...].astype(F32) + r_ref[i].astype(F32)
        out[...] = jnp.where(s < HALF, total, o[...].astype(F32)).astype(BF16)


def edge(fields, out, back, grads, gout, skip, first):
    _, _, width = fields.shape
    n = back.shape[1] // skip
    at = pl.BlockSpec((skip, SUB, width), lambda i: (i + first, 0, 0))
    strip = pl.BlockSpec((2, skip, SUB, width), lambda i: (0, i, 0, 0))
    return pl.pallas_call(
        edge_kernel,
        grid=(n,),
        in_specs=[at, at, strip, at, at],
        out_specs=[at, at],
        out_shape=(jax.ShapeDtypeStruct(out.shape, BF16),) * 2,
        input_output_aliases={1: 0, 4: 1},
        name="edge",
    )(fields, out, back, grads, gout)


def rim_kernel(f_ref, low_ref, c_ref, g_ref, out_any, gout_any, out_ref, gout_ref):
    for i, (f, out) in enumerate(((f_ref, out_ref), (g_ref, gout_ref))):
        back = low_ref[i].astype(F32)
        corner = c_ref[i].astype(F32)
        s = lax.broadcasted_iota(jnp.int32, corner.shape, 1)
        head = jnp.where(s < HALF, corner, back[:, :SUB])
        back = jnp.concatenate([head, back[:, SUB:]], axis=1)
        out[...] = (f[...].astype(F32) + back).astype(BF16)


def rim(fields, low, corner, grads, out, gout):
    _, skip, cols, width = low.shape
    at = pl.BlockSpec((skip, cols, width), lambda i: (0, 0, 0))
    whole = lambda *shape: pl.BlockSpec(shape, lambda i: (0,) * len(shape))
    anyw = pl.BlockSpec(memory_space=pl.ANY)
    return pl.pallas_call(
        rim_kernel,
        grid=(1,),
        in_specs=[at, whole(2, skip, cols, width), whole(2, skip, SUB, width), at, anyw, anyw],
        out_specs=[at, at],
        out_shape=(jax.ShapeDtypeStruct(out.shape, BF16),) * 2,
        input_output_aliases={4: 0, 5: 1},
        name="rim",
    )(fields, low, corner, grads, out, gout)


def linear(lon, lat, lats):
    return lon * lats + lat


def shift_by(block, step_lon, step_lat):
    lons, lats = lax.axis_size("lon"), lax.axis_size("lat")
    route = [
        (linear((i + step_lon) % lons, (j + step_lat) % lats, lats), linear(i, j, lats))
        for i in range(lons)
        for j in range(lats)
    ]
    return lax.ppermute(block, AXES, route)


def stages():
    lons, lats = lax.axis_size("lon"), lax.axis_size("lat")
    lat_bits = [1 << i for i in range(lats.bit_length() - 1)]
    lon_bits = [lats << i for i in range(lons.bit_length() - 1)]
    assert lats == 1 << len(lat_bits) and lons == 1 << len(lon_bits)
    far = lon_bits[1:]
    groups = [lat_bits[i : i + 2] for i in range(0, len(lat_bits), 2)]
    groups += [far[i : i + 2] for i in range(0, len(far), 2)]
    groups += [lon_bits[:1]]
    return groups, sorted(lat_bits + lon_bits)[::-1]


def swap(block, bit):
    total = lax.axis_size("lon") * lax.axis_size("lat")
    return lax.ppermute(block, AXES, [(i, i ^ bit) for i in range(total)])


def join(mine, other, bit, bits, place):
    high = (place & bit) != 0
    return jnp.concatenate(
        [jnp.where(high, other, mine), jnp.where(high, mine, other)], axis=bits.index(bit)
    )


def gather_stage(held, group, bits, place):
    if len(group) == 1:
        return join(held, swap(held, group[0]), group[0], bits, place)
    b1, b2 = group
    o1, o2, o3 = swap(held, b1), swap(held, b2), swap(held, b1 | b2)
    return join(join(held, o1, b1, bits, place), join(o2, o3, b1, bits, place), b2, bits, place)


def part_of(held, bit, bits, index):
    return lax.dynamic_index_in_dim(held, index, bits.index(bit), keepdims=True)


def scatter_stage(held, group, bits, place):
    here = [jnp.where((place & bit) != 0, 1, 0) for bit in group]
    total = held
    for bit, i in zip(group, here):
        total = part_of(total, bit, bits, i)
    total = total.astype(F32)
    for flips in range(1, 1 << len(group)):
        send, mask = held, 0
        for k, (bit, i) in enumerate(zip(group, here)):
            flip = (flips >> k) & 1
            send = part_of(send, bit, bits, 1 - i if flip else i)
            mask |= bit * flip
        total = total + swap(send.astype(BF16), mask).astype(F32)
    return total


def lines_of(grid):
    rows, cols, levels, width = grid.shape
    return grid.transpose(0, 2, 1, 3).reshape(rows * levels, cols, width)


def grid_of(lines, levels):
    count, cols, width = lines.shape
    return lines.reshape(count // levels, levels, cols, width).transpose(0, 2, 1, 3)


def paired(lines):
    *lead, count, cols, width = lines.shape
    return lines.reshape(*lead, count // 2, 2 * cols, width)


def unpaired(pairs):
    *lead, count, cols, width = pairs.shape
    return pairs.reshape(*lead, count * 2, cols // 2, width)


def block(fields, region_ids, w_qkv, w_proj, grad_output):
    rows, cols, levels, width = fields.shape
    skip = HALF * levels // 2
    devices = lax.axis_size("lon") * lax.axis_size("lat")
    factor = float(rows * cols * levels * devices) ** (-0.5)
    place = lax.axis_index(AXES)
    groups, bits = stages()
    share = w_qkv.shape[0]
    f_lines, g_lines = lines_of(fields), lines_of(grad_output)
    f_pairs, g_pairs = paired(f_lines), paired(g_lines)
    held = jnp.concatenate([w_qkv, w_proj], axis=0)
    held = held.reshape((1,) * len(bits) + held.shape)
    for group in groups:
        held = gather_stage(held, group, bits, place)
    held = held.reshape(devices, -1, width)
    w3 = held[:, :share].reshape(3, width, width)
    p_all = held[:, share:].reshape(width, width)
    both = jnp.stack
    low = shift_by(both([f_lines[: 2 * skip], g_lines[: 2 * skip]]), 0, 1)
    east = shift_by(both([f_lines[2 * skip :, :SUB], g_lines[2 * skip :, :SUB]]), 1, 0)
    corner = shift_by(both([f_lines[: 2 * skip, :SUB], g_lines[: 2 * skip, :SUB]]), 1, 1)
    low, east, corner = paired(low), paired(east), paired(corner)
    regions = token_regions(region_ids, levels)
    n00, i00, g00 = assemble_own(f_pairs, g_pairs, skip)
    a00, q00, *carry = attention(n00, g00, regions[0, :1], w3, p_all)
    n1, i1, g1 = assemble_low(f_pairs, g_pairs, east, low, corner, skip)
    a1, q1, *carry = attention(n1, g1, regions[1], w3, p_all, carry)
    n01, i01, g01 = assemble_east(f_pairs, g_pairs, east, skip)
    set1 = (a1, q1, n1, i1)
    out, gout, r_east1, r_low, r_corner = finish(
        (set1, set1), (0, 1), w3, p_all, f_pairs, g_pairs, skip, True
    )
    r_low = shift_by(unpaired(r_low), 0, -1)
    r_corner = shift_by(unpaired(r_corner), -1, -1)
    r_east1 = shift_by(unpaired(r_east1), -1, 0)
    a01, q01, grad_w, grad_p = attention(n01, g01, regions[0, 1:], w3, p_all, carry, True)
    grads = jnp.concatenate(
        [grad_w.reshape(devices, -1, width), grad_p.reshape(devices, -1, width)], axis=1
    )
    grads = grads.reshape((2,) * len(bits) + grads.shape[1:])
    for group in groups[::-1]:
        grads = scatter_stage(grads, group, bits, place)
    grads = grads.reshape(-1, width) * factor
    out, gout, r_east0 = finish(
        ((a00, q00, n00, i00), (a01, q01, n01, i01)), (0, 0), w3, p_all, f_pairs, g_pairs,
        skip, False, (out, gout),
    )
    r_east0 = shift_by(unpaired(r_east0), -1, 0)
    out, gout = unpaired(out), unpaired(gout)
    out, gout = rim(f_lines, r_low, r_corner, g_lines, out, gout)
    out, gout = edge(f_lines, out, r_east1, g_lines, gout, 2 * skip, rows * levels // (2 * skip) - 1)
    out, gout = edge(f_lines, out, r_east0, g_lines, gout, 2 * skip, 1)
    return (grid_of(out, levels), grid_of(gout, levels), grads[:share], grads[share:])


def solution(mesh):
    return jax.shard_map(
        block,
        mesh=mesh,
        in_specs=(
            P("lat", "lon", None, None),
            P("lat"),
            P(AXES, None),
            P(AXES, None),
            P("lat", "lon", None, None),
        ),
        out_specs=(
            P("lat", "lon", None, None),
            P("lat", "lon", None, None),
            P(AXES, None),
            P(AXES, None),
        ),
        check_vma=False,
    )
```

```python
import functools

import jax
import jax.numpy as jnp
from jax import lax
from jax.experimental import pallas as pl
from jax.experimental.pallas import tpu as pltpu
from jax.sharding import PartitionSpec as P


HEAD = 64
WIN = 12
HALF = WIN // 2
EPSILON = 1e-05
AXES = ("lon", "lat")
LANES = 128
SUB = 8


F32 = jnp.float32
BF16 = jnp.bfloat16


def nt(a, b):
    return lax.dot_general(a, b, (((1,), (1,)), ((), ())), preferred_element_type=F32)


def nn(a, b):
    return lax.dot_general(a, b, (((1,), (0,)), ((), ())), preferred_element_type=F32)


GROUP = 2


def sub_index(width):
    return lax.broadcasted_iota(jnp.int32, (SUB, width), 0)


def pick_first(own):
    s = sub_index(own.shape[1])
    t0a, t1a, t2a, t0b, t1b, t2b = [own[8 * i : 8 * i + 8] for i in range(6)]
    mixed = jnp.where(
        s < 2,
        t2a,
        jnp.where(s < 4, pltpu.roll(t2b, 2, 0), jnp.where(s < 6, pltpu.roll(t0b, 6, 0), t0a)),
    )
    return jnp.concatenate([t1a, t1b, mixed], axis=0)


def pick_second(own, strip):
    s = sub_index(own.shape[1])
    t2a, t2b = own[16:24], own[40:48]
    ha, hb = strip[:8], strip[8:]
    n1 = jnp.where(s < 2, ha, t2a)
    n2 = jnp.where(s < 2, hb, t2b)
    n3 = jnp.where((s >= 2) & (s < 6), ha, pltpu.roll(hb, 4, 0))
    return jnp.concatenate([n1, n2, n3], axis=0)


def unpick(first, second):
    s = sub_index(first.shape[1])
    t1a, t1b, mixed = first[:8], first[8:16], first[16:]
    n1, n2, n3 = second[:8], second[8:16], second[16:]
    zero = jnp.zeros_like(mixed)
    t0a = jnp.where(s >= 6, mixed, zero)
    t0b = jnp.where(s >= 6, pltpu.roll(mixed, 2, 0), zero)
    t2a = jnp.where(s < 2, mixed, n1)
    t2b = jnp.where(s < 2, pltpu.roll(mixed, 6, 0), n2)
    ha = jnp.where(s < 2, n1, n3)
    hb = jnp.where(s < 2, n2, pltpu.roll(n3, 4, 0))
    own = jnp.concatenate([t0a, t1a, t2a, t0b, t1b, t2b], axis=0)
    return own, jnp.concatenate([ha, hb], axis=0)


def token_regions(region_ids, levels):
    lines = jnp.repeat(region_ids, levels)
    pairs = lines.reshape(-1, 2)
    s = jnp.arange(3 * SUB)
    inner = s % SUB
    line0 = jnp.where(s < 8, 0, jnp.where(s < 16, 1, jnp.where((inner < 2) | (inner >= 6), 0, 1)))
    line1 = jnp.where(s < 8, 0, jnp.where(s < 16, 1, jnp.where((inner >= 2) & (inner < 6), 0, 1)))
    a, b = pairs[:, :1], pairs[:, 1:]
    both = jnp.stack([jnp.where(line0 == 0, a, b), jnp.where(line1 == 0, a, b)])
    per_band = WIN * levels // 2
    bands = pairs.shape[0] // per_band
    return both.reshape(2, bands, per_band * 3 * SUB).transpose(1, 0, 2)


def pack_kernel(f_ref, f_first, g_ref, g_first, low_ref, corner_ref, east_ref):
    n = low_ref.shape[1]
    for i, (x, first) in enumerate(((f_ref, f_first), (g_ref, g_first))):
        low_ref[i] = x[...]
        corner_ref[i] = first[:n]
        east_ref[i] = first[n:]


def pack(f_lines, g_lines, n):
    lines, cols, width = f_lines.shape
    low = pl.BlockSpec((n, cols, width), lambda i: (0, 0, 0))
    first = pl.BlockSpec((lines, SUB, width), lambda i: (0, 0, 0))
    shapes = [(2, n, cols, width), (2, n, SUB, width), (2, lines - n, SUB, width)]
    return pl.pallas_call(
        pack_kernel,
        grid=(1,),
        in_specs=[low, first, low, first],
        out_specs=[pl.BlockSpec(shape, lambda i: (0,) * 4) for shape in shapes],
        out_shape=tuple(jax.ShapeDtypeStruct(shape, BF16) for shape in shapes),
        name="pack",
    )(f_lines, f_lines, g_lines, g_lines)


def norm(block):
    centre = block - jnp.mean(block, axis=-1, keepdims=True)
    inverse = lax.rsqrt(jnp.mean(centre * centre, axis=-1, keepdims=True) + EPSILON)
    return (centre * inverse).astype(BF16), inverse


def put(at, p, block, grads, normed_ref, inv_ref, gs_ref):
    normed, inverse = norm(block)
    normed_ref[at, p] = normed
    inv_ref[at, p] = jnp.broadcast_to(inverse, (3 * SUB, LANES))
    gs_ref[at, p] = grads.astype(BF16)


def assemble_own_kernel(f_ref, g_ref, *outs):
    @pl.loop(0, f_ref.shape[0], unroll=3)
    def _(p):
        put(0, p, pick_first(f_ref[p].astype(F32)), pick_first(g_ref[p].astype(F32)), *outs)


def assemble_below_kernel(f_ref, g_ref, low_ref, *outs):
    @pl.when(pl.program_id(0) == 0)
    def _():
        @pl.loop(0, f_ref.shape[0], unroll=3)
        def _(p):
            put(0, p, pick_first(f_ref[p].astype(F32)), pick_first(g_ref[p].astype(F32)), *outs)

    @pl.when(pl.program_id(0) == 1)
    def _():
        @pl.loop(0, f_ref.shape[0], unroll=3)
        def _(p):
            put(0, p, pick_first(low_ref[0, p].astype(F32)), pick_first(low_ref[1, p].astype(F32)), *outs)


def assemble_second_kernel(f_ref, g_ref, east_ref, low_ref, corner_ref, *outs):
    last = pl.num_programs(0) - 1

    @pl.when(pl.program_id(0) < last)
    def _():
        @pl.loop(0, f_ref.shape[0], unroll=3)
        def _(p):
            put(
                0,
                p,
                pick_second(f_ref[p].astype(F32), east_ref[0, p].astype(F32)),
                pick_second(g_ref[p].astype(F32), east_ref[1, p].astype(F32)),
                *outs,
            )

    @pl.when(pl.program_id(0) == last)
    def _():
        @pl.loop(0, f_ref.shape[0], unroll=3)
        def _(p):
            put(
                0,
                p,
                pick_second(low_ref[0, p].astype(F32), corner_ref[0, p].astype(F32)),
                pick_second(low_ref[1, p].astype(F32), corner_ref[1, p].astype(F32)),
                *outs,
            )


def assembled(kernel, windows, skip, width, specs, args):
    shape = (windows, 2 * skip, 3 * SUB)
    out = lambda w: pl.BlockSpec((1, skip, 3 * SUB, w), lambda s: (s // 2, s % 2, 0, 0))
    outs = pl.pallas_call(
        kernel,
        grid=(2 * windows,),
        in_specs=specs,
        out_specs=[out(width), out(LANES), out(width)],
        out_shape=(
            jax.ShapeDtypeStruct(shape + (width,), BF16),
            jax.ShapeDtypeStruct(shape + (LANES,), F32),
            jax.ShapeDtypeStruct(shape + (width,), BF16),
        ),
        cost_estimate=pl.CostEstimate(
            flops=windows * skip * 3 * SUB * width * 100, transcendentals=0,
            bytes_accessed=windows * skip * 3 * SUB * width * 16),
    )(*args)
    count = 2 * skip * 3 * SUB
    return [x.reshape(windows, count, x.shape[-1]) for x in outs]


def assemble_own(fields, grads, skip):
    width = fields.shape[2]
    own = pl.BlockSpec((skip, 48, width), lambda s: (s + 1, 0, 0))
    return assembled(assemble_own_kernel, 1, skip, width, [own, own], (fields, grads))


def assemble_below(fields, grads, low, skip):
    width = fields.shape[2]
    last = fields.shape[0] // skip - 1
    own = pl.BlockSpec((skip, 48, width), lambda s: (last, 0, 0))
    below = pl.BlockSpec((2, skip, 48, width), lambda s: (0, 0, 0, 0))
    return assembled(assemble_below_kernel, 1, skip, width, [own, own, below], (fields, grads, low))


def assemble_second(fields, grads, east, low, corner, skip):
    width = fields.shape[2]
    n = fields.shape[0] // skip - 1
    own = pl.BlockSpec((skip, 48, width), lambda s: (jnp.minimum(s + 1, n), 0, 0))
    strip = pl.BlockSpec((2, skip, 16, width), lambda s: (0, jnp.minimum(s, n - 1), 0, 0))
    below = pl.BlockSpec((2, skip, 48, width), lambda s: (0, 0, 0, 0))
    diagonal = pl.BlockSpec((2, skip, 16, width), lambda s: (0, 0, 0, 0))
    return assembled(
        assemble_second_kernel, (n + 1) // 2, skip, width, [own, own, strip, below, diagonal],
        (fields, grads, east, low, corner),
    )


def attention_kernel(*refs, first, carried, into):
    normed_ref, gs_ref, reg_ref, w_ref, wp_ref = refs[:5]
    refs = refs[5:]
    if carried:
        gw_in, gp_in = refs[:2]
        refs = refs[2 + (2 if into else 0):]
    att_ref, gqkv_ref, gw_ref, gp_ref = refs
    group = pl.program_id(0) + first
    window = pl.program_id(1)
    scale = HEAD ** (-0.5)
    normed = normed_ref[window]
    grads = gs_ref[window]
    count = normed.shape[0]
    wide = GROUP * LANES
    weights = w_ref[...].reshape(3 * wide, w_ref.shape[2])
    qkv = nt(normed, weights).astype(BF16)
    queries, all_keys, all_values = [qkv[:, wide * i : wide * (i + 1)] for i in range(3)]
    queries = queries * jnp.asarray(scale, BF16)
    grad_att_all = nn(grads, wp_ref[...]).astype(BF16)
    all_keys_t = all_keys.astype(F32).T.astype(BF16) * jnp.asarray(scale, BF16)
    all_values_t = all_values.astype(F32).T.astype(BF16)
    region = reg_ref[window]
    region_t = jnp.broadcast_to(region, (LANES, count)).T
    spread = jnp.concatenate([region_t] * -(-count // LANES), axis=1)[:, :count]
    allowed = spread == region
    lane = lax.broadcasted_iota(jnp.int32, (count, LANES), 1)
    zero = jnp.zeros((), BF16)
    att_t, grad_q_t, grad_ks, grad_vs = [], [], [], []
    for pair in range(GROUP):
        cols = slice(pair * LANES, (pair + 1) * LANES)
        query, keys, values = queries[:, cols], all_keys[:, cols], all_values[:, cols]
        keys_t, values_t = all_keys_t[cols], all_values_t[cols]
        grad_att = grad_att_all[:, cols]
        grad_k = grad_v = None
        for h in range(LANES // HEAD):
            mine = (lane >= h * HEAD) & (lane < (h + 1) * HEAD)
            rows = slice(h * HEAD, (h + 1) * HEAD)
            scores = nt(jnp.where(mine, keys, zero), query)
            scores = jnp.where(allowed, scores, -1e30)
            peak = jnp.max(scores, axis=0, keepdims=True)
            expo = jnp.exp(scores - peak)
            ratio = 1.0 / jnp.sum(expo, axis=0, keepdims=True)
            rounded = (expo * ratio).astype(BF16)
            grad_probs = nt(jnp.where(mine, values, zero), grad_att)
            att_t.append(nn(values_t[rows], rounded))
            inner = jnp.sum(grad_probs * expo, axis=0, keepdims=True) * ratio
            grad_scores = (expo * (grad_probs - inner) * ratio).astype(BF16)
            grad_q_t.append(nn(keys_t[rows], grad_scores))
            part_v = nn(rounded, jnp.where(mine, grad_att, zero))
            part_k = nn(grad_scores, jnp.where(mine, query, zero))
            grad_k = part_k if grad_k is None else grad_k + part_k
            grad_v = part_v if grad_v is None else grad_v + part_v
        grad_ks.append(grad_k)
        grad_vs.append(grad_v)
    att_t = jnp.concatenate(att_t, axis=0)
    grad_q_t = jnp.concatenate(grad_q_t, axis=0)
    grad_k = jnp.concatenate(grad_ks, axis=1)
    grad_v = jnp.concatenate(grad_vs, axis=1)
    att_ref[0] = att_t.T.astype(BF16)
    gqkv_ref[0, 0] = grad_q_t.T.astype(BF16)
    gqkv_ref[0, 1] = grad_k.astype(BF16)
    gqkv_ref[0, 2] = grad_v.astype(BF16)
    turned = [grad_q_t.astype(BF16), grad_k.T.astype(BF16), grad_v.T.astype(BF16)]
    grad_w = nn(jnp.concatenate(turned, axis=0), normed).reshape(3, wide, grads.shape[1])
    grad_p = nn(att_t.astype(BF16), grads).T

    def start(add):
        gw_ref[...] = grad_w + gw_in[...] if add else grad_w
        gp_ref[...] = grad_p + gp_in[...] if add else grad_p

    opening = window == 0
    if carried:
        pl.when(opening & (group < carried))(lambda: start(True))
    pl.when(opening & (group >= carried))(lambda: start(False))

    @pl.when(window > 0)
    def _():
        gw_ref[...] += grad_w
        gp_ref[...] += grad_p


def attention(normed, gs, regions, w_qkv, w_proj, carry=(), carried=0, groups=None, into=()):
    windows, count, width = normed.shape
    wide = GROUP * LANES
    first, number = groups or (0, width // wide)
    whole = lambda *shape: pl.BlockSpec(shape, lambda p, w: (0,) * len(shape))
    rows3 = pl.BlockSpec((3, wide, width), lambda p, w: (0, p + first, 0))
    cols1 = pl.BlockSpec((width, wide), lambda p, w: (0, p + first))
    anyw = pl.BlockSpec(memory_space=pl.ANY)
    args = [normed, gs, regions[:, None, :], w_qkv, w_proj, *carry, *into]
    alias = {}
    if carry:
        alias = {5: 2, 6: 3}
    if into:
        alias |= {7: 0, 8: 1}
    return pl.pallas_call(
        functools.partial(attention_kernel, first=first, carried=carried, into=bool(into)),
        grid=(number, windows),
        in_specs=[
            whole(windows, count, width),
            whole(windows, count, width),
            whole(windows, 1, count),
            rows3,
            cols1,
        ]
        + ([rows3, cols1] if carry else [])
        + ([anyw, anyw] if into else []),
        out_specs=[
            pl.BlockSpec((1, count, wide), lambda p, w: (w, 0, p + first)),
            pl.BlockSpec((1, 3, count, wide), lambda p, w: (w, 0, 0, p + first)),
            rows3,
            cols1,
        ],
        out_shape=(
            jax.ShapeDtypeStruct((windows, count, width), BF16),
            jax.ShapeDtypeStruct((windows, 3, count, width), BF16),
            jax.ShapeDtypeStruct((3, width, width), F32),
            jax.ShapeDtypeStruct((width, width), F32),
        ),
        input_output_aliases=alias,
        cost_estimate=pl.CostEstimate(
            flops=windows * count * number * wide * (16 * width + 12 * count), transcendentals=0,
            bytes_accessed=windows * count * number * wide * 12),
    )(*args)


def back(att, gqkv, normed, inv, w_ref, wp_ref, scr):
    shape = scr.shape[1:]
    branch = nt(att[0], wp_ref[...])
    scr[0] = branch.astype(BF16).astype(F32).reshape(shape)
    grad_normed = nn(gqkv[0, 0], w_ref[0]) + nn(gqkv[0, 1], w_ref[1]) + nn(gqkv[0, 2], w_ref[2])
    normal = normed[0].astype(F32)
    mean = jnp.mean(grad_normed, axis=-1, keepdims=True)
    along = jnp.mean(grad_normed * normal, axis=-1, keepdims=True)
    pre = inv[0][:, :1] * (grad_normed - mean - normal * along)
    scr[1] = pre.astype(BF16).astype(F32).reshape(shape)


def finish_low_kernel(*refs):
    ins, (w_ref, wp_ref, f_ref, g_ref) = refs[:8], refs[8:12]
    out_ref, gout_ref, east_ref, low_ref, corner_ref, first, second = refs[12:]
    back(*ins[:4], w_ref, wp_ref, first)
    back(*ins[4:], w_ref, wp_ref, second)
    n = f_ref.shape[0]

    @pl.when(pl.program_id(0) == 0)
    def _():
        @pl.loop(0, n, unroll=3)
        def _(p):
            for i, (x, o) in enumerate(((f_ref, out_ref), (g_ref, gout_ref))):
                add, strip = unpick(first[i, p], second[i, p])
                o[p] = (x[p].astype(F32) + add).astype(BF16)
                east_ref[i, p] = strip.astype(BF16)

    @pl.when(pl.program_id(0) == 1)
    def _():
        @pl.loop(0, n, unroll=3)
        def _(p):
            for i in range(2):
                add, strip = unpick(first[i, p], second[i, p])
                low_ref[i, p] = add.astype(BF16)
                corner_ref[i, p] = strip.astype(BF16)


def finish_east_kernel(att, gqkv, normed, inv, w_ref, wp_ref, east_ref, kept_ref, second):
    back(att, gqkv, normed, inv, w_ref, wp_ref, second)
    kept_ref[...] = second[...].astype(BF16)

    @pl.loop(0, second.shape[1], unroll=3)
    def _(p):
        for i in range(2):
            _, strip = unpick(second[i, p], second[i, p])
            east_ref[i, p] = strip.astype(BF16)


def finish_top_kernel(att, gqkv, normed, inv, kept_ref, w_ref, wp_ref, f_ref, g_ref, any0, any1,
                      out_ref, gout_ref, first):
    back(att, gqkv, normed, inv, w_ref, wp_ref, first)

    @pl.loop(0, f_ref.shape[0], unroll=3)
    def _(p):
        for i, (x, o) in enumerate(((f_ref, out_ref), (g_ref, gout_ref))):
            add, _ = unpick(first[i, p], kept_ref[i, p].astype(F32))
            o[p] = (x[p].astype(F32) + add).astype(BF16)


def finish_call(kernel, sets, width, skip, w_qkv, w_proj, more, specs, outs, out_specs, alias,
                ahead=()):
    part = skip * 3 * SUB
    whole = lambda *shape: pl.BlockSpec(shape, lambda s: (0,) * len(shape))
    ins, args = [], []
    for at, arrays in sets:
        ins += [
            pl.BlockSpec((1, part, width), lambda s, at=at: (at, s, 0)),
            pl.BlockSpec((1, 3, part, width), lambda s, at=at: (at, 0, s, 0)),
            pl.BlockSpec((1, part, width), lambda s, at=at: (at, s, 0)),
            pl.BlockSpec((1, part, LANES), lambda s, at=at: (at, s, 0)),
        ]
        args += arrays
    args += [x for x, _ in ahead] + [w_qkv, w_proj] + list(more)
    ins += [x for _, x in ahead] + [whole(3, width, width), whole(width, width)] + list(specs)
    return pl.pallas_call(
        kernel,
        grid=(2,),
        in_specs=ins,
        out_specs=out_specs,
        out_shape=tuple(jax.ShapeDtypeStruct(shape, BF16) for shape in outs),
        scratch_shapes=[pltpu.VMEM((2, skip, 3 * SUB, width), F32)] * len(sets),
        input_output_aliases={len(args) - back_at: at for back_at, at in alias.items()},
        cost_estimate=pl.CostEstimate(
            flops=2 * len(sets) * part * 8 * width * width, transcendentals=0,
            bytes_accessed=4 * len(sets) * part * width * 16),
    )(*args)


def finish_low(first, second, w_qkv, w_proj, fields, grads, skip):
    pairs, _, width = fields.shape
    last = pairs // skip - 1
    own = pl.BlockSpec((skip, 48, width), lambda s: (last, 0, 0))
    whole = lambda *shape: pl.BlockSpec(shape, lambda s: (0,) * len(shape))
    strips = [(2, skip, 16, width), (2, skip, 48, width), (2, skip, 16, width)]
    return finish_call(
        finish_low_kernel, [(0, first), (1, second)], width, skip, w_qkv, w_proj,
        (fields, grads), (own, own), [(pairs, 48, width)] * 2 + strips,
        [own, own] + [whole(*shape) for shape in strips], {},
    )


def finish_east(arrays, w_qkv, w_proj, skip):
    width = w_proj.shape[0]
    rows = lambda n: pl.BlockSpec((2, skip, n, width), lambda s: (0, s, 0, 0))
    return finish_call(
        finish_east_kernel, [(0, arrays)], width, skip, w_qkv, w_proj, (), (),
        [(2, 2 * skip, 16, width), (2, 2 * skip, 3 * SUB, width)],
        [rows(16), rows(3 * SUB)], {},
    )


def finish_top(arrays, kept, w_qkv, w_proj, fields, grads, skip, into):
    pairs, _, width = fields.shape
    own = pl.BlockSpec((skip, 48, width), lambda s: (s + 1, 0, 0))
    anyw = pl.BlockSpec(memory_space=pl.ANY)
    rows = pl.BlockSpec((2, skip, 3 * SUB, width), lambda s: (0, s, 0, 0))
    return finish_call(
        finish_top_kernel, [(0, arrays)], width, skip, w_qkv, w_proj,
        (fields, grads, *into), (own, own, anyw, anyw), [(pairs, 48, width)] * 2,
        [own, own], {2: 0, 1: 1}, ahead=[(kept, rows)],
    )


def edge_kernel(f_ref, o_ref, r_ref, g_ref, q_ref, out_ref, gout_ref):
    s = lax.broadcasted_iota(jnp.int32, f_ref.shape, 1)
    for i, (f, o, out) in enumerate(((f_ref, o_ref, out_ref), (g_ref, q_ref, gout_ref))):
        total = f[...].astype(F32) + r_ref[i].astype(F32)
        out[...] = jnp.where(s < HALF, total, o[...].astype(F32)).astype(BF16)


def edge(fields, out, back, grads, gout, skip, first):
    _, _, width = fields.shape
    n = back.shape[1] // skip
    at = pl.BlockSpec((skip, SUB, width), lambda i: (i + first, 0, 0))
    strip = pl.BlockSpec((2, skip, SUB, width), lambda i: (0, i, 0, 0))
    return pl.pallas_call(
        edge_kernel,
        grid=(n,),
        in_specs=[at, at, strip, at, at],
        out_specs=[at, at],
        out_shape=(jax.ShapeDtypeStruct(out.shape, BF16),) * 2,
        input_output_aliases={1: 0, 4: 1},
        name="edge",
    )(fields, out, back, grads, gout)


def rim_kernel(f_ref, low_ref, c_ref, g_ref, out_any, gout_any, out_ref, gout_ref):
    for i, (f, out) in enumerate(((f_ref, out_ref), (g_ref, gout_ref))):
        back = low_ref[i].astype(F32)
        corner = c_ref[i].astype(F32)
        s = lax.broadcasted_iota(jnp.int32, corner.shape, 1)
        head = jnp.where(s < HALF, corner, back[:, :SUB])
        back = jnp.concatenate([head, back[:, SUB:]], axis=1)
        out[...] = (f[...].astype(F32) + back).astype(BF16)


def rim(fields, low, corner, grads, out, gout):
    _, skip, cols, width = low.shape
    at = pl.BlockSpec((skip, cols, width), lambda i: (0, 0, 0))
    whole = lambda *shape: pl.BlockSpec(shape, lambda i: (0,) * len(shape))
    anyw = pl.BlockSpec(memory_space=pl.ANY)
    return pl.pallas_call(
        rim_kernel,
        grid=(1,),
        in_specs=[at, whole(2, skip, cols, width), whole(2, skip, SUB, width), at, anyw, anyw],
        out_specs=[at, at],
        out_shape=(jax.ShapeDtypeStruct(out.shape, BF16),) * 2,
        input_output_aliases={4: 0, 5: 1},
        name="rim",
    )(fields, low, corner, grads, out, gout)


def linear(lon, lat, lats):
    return lon * lats + lat


def shift_by(block, step_lon, step_lat):
    lons, lats = lax.axis_size("lon"), lax.axis_size("lat")
    route = [
        (linear((i + step_lon) % lons, (j + step_lat) % lats, lats), linear(i, j, lats))
        for i in range(lons)
        for j in range(lats)
    ]
    return lax.ppermute(block, AXES, route)


def stages():
    lons, lats = lax.axis_size("lon"), lax.axis_size("lat")
    lat_bits = [1 << i for i in range(lats.bit_length() - 1)]
    lon_bits = [lats << i for i in range(lons.bit_length() - 1)]
    assert lats == 1 << len(lat_bits) and lons == 1 << len(lon_bits)
    far = lon_bits[1:]
    groups = [lat_bits[i : i + 2] for i in range(0, len(lat_bits), 2)]
    groups += [far[i : i + 2] for i in range(0, len(far), 2)]
    groups += [lon_bits[:1]]
    return groups, sorted(lat_bits + lon_bits)[::-1]


def swap(block, bit):
    total = lax.axis_size("lon") * lax.axis_size("lat")
    return lax.ppermute(block, AXES, [(i, i ^ bit) for i in range(total)])


def join(mine, other, bit, bits, place):
    high = (place & bit) != 0
    axis = bits.index(bit)
    return jnp.where(
        high,
        jnp.concatenate([other, mine], axis=axis),
        jnp.concatenate([mine, other], axis=axis),
    )


def gather_stage(held, group, bits, place):
    if len(group) == 1:
        return join(held, swap(held, group[0]), group[0], bits, place)
    b1, b2 = group
    o1, o2, o3 = swap(held, b1), swap(held, b2), swap(held, b1 | b2)
    return join(join(held, o1, b1, bits, place), join(o2, o3, b1, bits, place), b2, bits, place)


def part_of(held, bit, bits, index):
    return lax.dynamic_index_in_dim(held, index, bits.index(bit), keepdims=True)


def scatter_stage(held, group, bits, place):
    here = [jnp.where((place & bit) != 0, 1, 0) for bit in group]
    total = held
    for bit, i in zip(group, here):
        total = part_of(total, bit, bits, i)
    total = total.astype(F32)
    for flips in range(1, 1 << len(group)):
        send, mask = held, 0
        for k, (bit, i) in enumerate(zip(group, here)):
            flip = (flips >> k) & 1
            send = part_of(send, bit, bits, 1 - i if flip else i)
            mask |= bit * flip
        total = total + swap(send.astype(BF16), mask).astype(F32)
    return total


def lines_of(grid):
    rows, cols, levels, width = grid.shape
    return grid.transpose(0, 2, 1, 3).reshape(rows * levels, cols, width)


def grid_of(lines, levels):
    count, cols, width = lines.shape
    return lines.reshape(count // levels, levels, cols, width).transpose(0, 2, 1, 3)


def paired(lines):
    *lead, count, cols, width = lines.shape
    return lines.reshape(*lead, count // 2, 2 * cols, width)


def unpaired(pairs):
    *lead, count, cols, width = pairs.shape
    return pairs.reshape(*lead, count * 2, cols // 2, width)


def block(fields, region_ids, w_qkv, w_proj, grad_output):
    rows, cols, levels, width = fields.shape
    skip = HALF * levels // 2
    devices = lax.axis_size("lon") * lax.axis_size("lat")
    factor = float(rows * cols * levels * devices) ** (-0.5)
    place = lax.axis_index(AXES)
    groups, bits = stages()
    share = w_qkv.shape[0]
    f_lines, g_lines = lines_of(fields), lines_of(grad_output)
    f_pairs, g_pairs = paired(f_lines), paired(g_lines)
    held = jnp.concatenate([w_qkv, w_proj], axis=0)
    held = held.reshape((1,) * len(bits) + held.shape)
    for group in groups[:-1]:
        held = gather_stage(held, group, bits, place)
    bit = groups[-1][0]
    other = swap(held, bit)
    w3 = join(held[..., :share, :], other[..., :share, :], bit, bits, place).reshape(3, width, width)
    p_all = join(held[..., share:, :], other[..., share:, :], bit, bits, place).reshape(width, width)
    low, corner, east = pack(f_lines, g_lines, 2 * skip)
    low = shift_by(low, 0, 1)
    east = shift_by(east, 1, 0)
    corner = shift_by(corner, 1, 1)
    low, east, corner = paired(low), paired(east), paired(corner)
    regions = token_regions(region_ids, levels)
    n00, i00, g00 = assemble_own(f_pairs, g_pairs, skip)
    n10, i10, g10 = assemble_below(f_pairs, g_pairs, low, skip)
    a10, q10, *carry = attention(n10, g10, regions[1, :1], w3, p_all)
    n1, i1, g1 = assemble_second(f_pairs, g_pairs, east, low, corner, skip)
    many = width // (GROUP * LANES)
    a1, q1, *carry = attention(n1, g1, regions[:, 1], w3, p_all, carry, many)
    out, gout, r_east1, r_low, r_corner = finish_low(
        (a10, q10, n10, i10), (a1, q1, n1, i1), w3, p_all, f_pairs, g_pairs, skip
    )
    r_low = shift_by(unpaired(r_low), 0, -1)
    r_corner = shift_by(unpaired(r_corner), -1, -1)
    r_east0, kept = finish_east((a1, q1, n1, i1), w3, p_all, skip)
    r_east1 = shift_by(unpaired(r_east1), -1, 0)
    r_east0 = shift_by(unpaired(r_east0), -1, 0)
    a00, q00, grad_w, grad_p = attention(n00, g00, regions[0, :1], w3, p_all, carry, many)
    grads = jnp.concatenate(
        [grad_w.reshape(devices, -1, width), grad_p.reshape(devices, -1, width)], axis=1
    )
    grads = grads.reshape((2,) * len(bits) + grads.shape[1:])
    for group in groups[::-1]:
        grads = scatter_stage(grads, group, bits, place)
    grads = grads.reshape(-1, width) * factor
    out, gout = finish_top(
        (a00, q00, n00, i00), kept, w3, p_all, f_pairs, g_pairs, skip, (out, gout)
    )
    out, gout = unpaired(out), unpaired(gout)
    out, gout = rim(f_lines, r_low, r_corner, g_lines, out, gout)
    out, gout = edge(f_lines, out, r_east1, g_lines, gout, 2 * skip, rows * levels // (2 * skip) - 1)
    out, gout = edge(f_lines, out, r_east0, g_lines, gout, 2 * skip, 1)
    return (grid_of(out, levels), grid_of(gout, levels), grads[:share], grads[share:])


def solution(mesh):
    return jax.shard_map(
        block,
        mesh=mesh,
        in_specs=(
            P("lat", "lon", None, None),
            P("lat"),
            P(AXES, None),
            P(AXES, None),
            P("lat", "lon", None, None),
        ),
        out_specs=(
            P("lat", "lon", None, None),
            P("lat", "lon", None, None),
            P(AXES, None),
            P(AXES, None),
        ),
        check_vma=False,
    )
```

```python
import functools

import jax
import jax.numpy as jnp
from jax import lax
from jax.experimental import pallas as pl
from jax.experimental.pallas import tpu as pltpu
from jax.sharding import PartitionSpec as P


HEAD = 64
WIN = 12
HALF = WIN // 2
EPSILON = 1e-05
AXES = ("lon", "lat")
LANES = 128
SUB = 8


F32 = jnp.float32
BF16 = jnp.bfloat16


def nt(a, b):
    return lax.dot_general(a, b, (((1,), (1,)), ((), ())), preferred_element_type=F32)


def nn(a, b):
    return lax.dot_general(a, b, (((1,), (0,)), ((), ())), preferred_element_type=F32)


GROUP = 2


def sub_index(width):
    return lax.broadcasted_iota(jnp.int32, (SUB, width), 0)


def pick_first(own):
    s = sub_index(own.shape[1])
    t0a, t1a, t2a, t0b, t1b, t2b = [own[8 * i : 8 * i + 8] for i in range(6)]
    mixed = jnp.where(
        s < 2,
        t2a,
        jnp.where(s < 4, pltpu.roll(t2b, 2, 0), jnp.where(s < 6, pltpu.roll(t0b, 6, 0), t0a)),
    )
    return jnp.concatenate([t1a, t1b, mixed], axis=0)


def pick_second(own, strip):
    s = sub_index(own.shape[1])
    t2a, t2b = own[16:24], own[40:48]
    ha, hb = strip[:8], strip[8:]
    n1 = jnp.where(s < 2, ha, t2a)
    n2 = jnp.where(s < 2, hb, t2b)
    n3 = jnp.where((s >= 2) & (s < 6), ha, pltpu.roll(hb, 4, 0))
    return jnp.concatenate([n1, n2, n3], axis=0)


def unpick(first, second):
    s = sub_index(first.shape[1])
    t1a, t1b, mixed = first[:8], first[8:16], first[16:]
    n1, n2, n3 = second[:8], second[8:16], second[16:]
    zero = jnp.zeros_like(mixed)
    t0a = jnp.where(s >= 6, mixed, zero)
    t0b = jnp.where(s >= 6, pltpu.roll(mixed, 2, 0), zero)
    t2a = jnp.where(s < 2, mixed, n1)
    t2b = jnp.where(s < 2, pltpu.roll(mixed, 6, 0), n2)
    ha = jnp.where(s < 2, n1, n3)
    hb = jnp.where(s < 2, n2, pltpu.roll(n3, 4, 0))
    own = jnp.concatenate([t0a, t1a, t2a, t0b, t1b, t2b], axis=0)
    return own, jnp.concatenate([ha, hb], axis=0)


def token_regions(region_ids, levels):
    lines = jnp.repeat(region_ids, levels)
    pairs = lines.reshape(-1, 2)
    s = jnp.arange(3 * SUB)
    inner = s % SUB
    line0 = jnp.where(s < 8, 0, jnp.where(s < 16, 1, jnp.where((inner < 2) | (inner >= 6), 0, 1)))
    line1 = jnp.where(s < 8, 0, jnp.where(s < 16, 1, jnp.where((inner >= 2) & (inner < 6), 0, 1)))
    a, b = pairs[:, :1], pairs[:, 1:]
    both = jnp.stack([jnp.where(line0 == 0, a, b), jnp.where(line1 == 0, a, b)])
    per_band = WIN * levels // 2
    bands = pairs.shape[0] // per_band
    return both.reshape(2, bands, per_band * 3 * SUB).transpose(1, 0, 2)


def pack_kernel(f_ref, f_first, g_ref, g_first, low_ref, corner_ref, east_ref):
    n = low_ref.shape[1]
    for i, (x, first) in enumerate(((f_ref, f_first), (g_ref, g_first))):
        low_ref[i] = x[...]
        corner_ref[i] = first[:n]
        east_ref[i] = first[n:]


def pack(f_lines, g_lines, n):
    lines, cols, width = f_lines.shape
    low = pl.BlockSpec((n, cols, width), lambda i: (0, 0, 0))
    first = pl.BlockSpec((lines, SUB, width), lambda i: (0, 0, 0))
    shapes = [(2, n, cols, width), (2, n, SUB, width), (2, lines - n, SUB, width)]
    return pl.pallas_call(
        pack_kernel,
        grid=(1,),
        in_specs=[low, first, low, first],
        out_specs=[pl.BlockSpec(shape, lambda i: (0,) * 4) for shape in shapes],
        out_shape=tuple(jax.ShapeDtypeStruct(shape, BF16) for shape in shapes),
        name="pack",
    )(f_lines, f_lines, g_lines, g_lines)


def norm(block):
    centre = block - jnp.mean(block, axis=-1, keepdims=True)
    inverse = lax.rsqrt(jnp.mean(centre * centre, axis=-1, keepdims=True) + EPSILON)
    return (centre * inverse).astype(BF16), inverse


def put(at, p, block, grads, normed_ref, inv_ref, gs_ref):
    normed, inverse = norm(block)
    normed_ref[at, p] = normed
    inv_ref[at, p] = jnp.broadcast_to(inverse, (3 * SUB, LANES))
    gs_ref[at, p] = grads.astype(BF16)


def assemble_own_kernel(f_ref, g_ref, *outs):
    @pl.loop(0, f_ref.shape[0], unroll=3)
    def _(p):
        put(0, p, pick_first(f_ref[p].astype(F32)), pick_first(g_ref[p].astype(F32)), *outs)


def assemble_below_kernel(f_ref, g_ref, low_ref, *outs):
    @pl.when(pl.program_id(0) == 0)
    def _():
        @pl.loop(0, f_ref.shape[0], unroll=3)
        def _(p):
            put(0, p, pick_first(f_ref[p].astype(F32)), pick_first(g_ref[p].astype(F32)), *outs)

    @pl.when(pl.program_id(0) == 1)
    def _():
        @pl.loop(0, f_ref.shape[0], unroll=3)
        def _(p):
            put(0, p, pick_first(low_ref[0, p].astype(F32)), pick_first(low_ref[1, p].astype(F32)), *outs)


def assemble_second_kernel(f_ref, g_ref, east_ref, low_ref, corner_ref, *outs):
    last = pl.num_programs(0) - 1

    @pl.when(pl.program_id(0) < last)
    def _():
        @pl.loop(0, f_ref.shape[0], unroll=3)
        def _(p):
            put(
                0,
                p,
                pick_second(f_ref[p].astype(F32), east_ref[0, p].astype(F32)),
                pick_second(g_ref[p].astype(F32), east_ref[1, p].astype(F32)),
                *outs,
            )

    @pl.when(pl.program_id(0) == last)
    def _():
        @pl.loop(0, f_ref.shape[0], unroll=3)
        def _(p):
            put(
                0,
                p,
                pick_second(low_ref[0, p].astype(F32), corner_ref[0, p].astype(F32)),
                pick_second(low_ref[1, p].astype(F32), corner_ref[1, p].astype(F32)),
                *outs,
            )


def assembled(kernel, windows, skip, width, specs, args):
    shape = (windows, 2 * skip, 3 * SUB)
    out = lambda w: pl.BlockSpec((1, skip, 3 * SUB, w), lambda s: (s // 2, s % 2, 0, 0))
    outs = pl.pallas_call(
        kernel,
        grid=(2 * windows,),
        in_specs=specs,
        out_specs=[out(width), out(LANES), out(width)],
        out_shape=(
            jax.ShapeDtypeStruct(shape + (width,), BF16),
            jax.ShapeDtypeStruct(shape + (LANES,), F32),
            jax.ShapeDtypeStruct(shape + (width,), BF16),
        ),
        cost_estimate=pl.CostEstimate(
            flops=windows * skip * 3 * SUB * width * 100, transcendentals=0,
            bytes_accessed=windows * skip * 3 * SUB * width * 16),
    )(*args)
    count = 2 * skip * 3 * SUB
    return [x.reshape(windows, count, x.shape[-1]) for x in outs]


def assemble_own(fields, grads, skip):
    width = fields.shape[2]
    own = pl.BlockSpec((skip, 48, width), lambda s: (s + 1, 0, 0))
    return assembled(assemble_own_kernel, 1, skip, width, [own, own], (fields, grads))


def assemble_below(fields, grads, low, skip):
    width = fields.shape[2]
    last = fields.shape[0] // skip - 1
    own = pl.BlockSpec((skip, 48, width), lambda s: (last, 0, 0))
    below = pl.BlockSpec((2, skip, 48, width), lambda s: (0, 0, 0, 0))
    return assembled(assemble_below_kernel, 1, skip, width, [own, own, below], (fields, grads, low))


def assemble_second(fields, grads, east, low, corner, skip):
    width = fields.shape[2]
    n = fields.shape[0] // skip - 1
    own = pl.BlockSpec((skip, 48, width), lambda s: (jnp.minimum(s + 1, n), 0, 0))
    strip = pl.BlockSpec((2, skip, 16, width), lambda s: (0, jnp.minimum(s, n - 1), 0, 0))
    below = pl.BlockSpec((2, skip, 48, width), lambda s: (0, 0, 0, 0))
    diagonal = pl.BlockSpec((2, skip, 16, width), lambda s: (0, 0, 0, 0))
    return assembled(
        assemble_second_kernel, (n + 1) // 2, skip, width, [own, own, strip, below, diagonal],
        (fields, grads, east, low, corner),
    )


def attention_kernel(*refs, carried, last):
    normed_ref, inv_ref, gs_ref, reg_ref, w_ref, wp_ref = refs[:6]
    refs = refs[6:]
    if carried:
        gw_in, gp_in = refs[:2]
        refs = refs[2:]
    back_ref, gw_ref, gp_ref, branch_acc, pre_acc = refs
    group = pl.program_id(0)
    window = pl.program_id(1)
    scale = HEAD ** (-0.5)
    normed = normed_ref[window]
    grads = gs_ref[window]
    count = normed.shape[0]
    wide = GROUP * LANES
    weights = w_ref[...].reshape(3 * wide, w_ref.shape[2])
    qkv = nt(normed, weights).astype(BF16)
    queries, all_keys, all_values = [qkv[:, wide * i : wide * (i + 1)] for i in range(3)]
    queries = queries * jnp.asarray(scale, BF16)
    grad_att_all = nn(grads, wp_ref[...]).astype(BF16)
    all_keys_t = all_keys.astype(F32).T.astype(BF16) * jnp.asarray(scale, BF16)
    all_values_t = all_values.astype(F32).T.astype(BF16)
    region = reg_ref[window]
    region_t = jnp.broadcast_to(region, (LANES, count)).T
    spread = jnp.concatenate([region_t] * -(-count // LANES), axis=1)[:, :count]
    allowed = spread == region
    lane = lax.broadcasted_iota(jnp.int32, (count, LANES), 1)
    zero = jnp.zeros((), BF16)
    att_t, grad_q_t, grad_ks, grad_vs = [], [], [], []
    for pair in range(GROUP):
        cols = slice(pair * LANES, (pair + 1) * LANES)
        query, keys, values = queries[:, cols], all_keys[:, cols], all_values[:, cols]
        keys_t, values_t = all_keys_t[cols], all_values_t[cols]
        grad_att = grad_att_all[:, cols]
        grad_k = grad_v = None
        for h in range(LANES // HEAD):
            mine = (lane >= h * HEAD) & (lane < (h + 1) * HEAD)
            rows = slice(h * HEAD, (h + 1) * HEAD)
            scores = nt(jnp.where(mine, keys, zero), query)
            scores = jnp.where(allowed, scores, -1e30)
            peak = jnp.max(scores, axis=0, keepdims=True)
            expo = jnp.exp(scores - peak)
            ratio = 1.0 / jnp.sum(expo, axis=0, keepdims=True)
            rounded = (expo * ratio).astype(BF16)
            grad_probs = nt(jnp.where(mine, values, zero), grad_att)
            att_t.append(nn(values_t[rows], rounded))
            inner = jnp.sum(grad_probs * expo, axis=0, keepdims=True) * ratio
            grad_scores = (expo * (grad_probs - inner) * ratio).astype(BF16)
            grad_q_t.append(nn(keys_t[rows], grad_scores))
            part_v = nn(rounded, jnp.where(mine, grad_att, zero))
            part_k = nn(grad_scores, jnp.where(mine, query, zero))
            grad_k = part_k if grad_k is None else grad_k + part_k
            grad_v = part_v if grad_v is None else grad_v + part_v
        grad_ks.append(grad_k)
        grad_vs.append(grad_v)
    att_t = jnp.concatenate(att_t, axis=0)
    grad_q_t = jnp.concatenate(grad_q_t, axis=0)
    grad_k = jnp.concatenate(grad_ks, axis=1)
    grad_v = jnp.concatenate(grad_vs, axis=1)
    att = att_t.T.astype(BF16)
    grad_qkv = jnp.concatenate(
        [grad_q_t.T.astype(BF16), grad_k.astype(BF16), grad_v.astype(BF16)], axis=1
    )
    branch = nt(att, wp_ref[...])
    grad_normed = nn(grad_qkv, weights)

    @pl.when(group == 0)
    def _():
        branch_acc[window] = branch
        pre_acc[window] = grad_normed

    @pl.when(group > 0)
    def _():
        branch_acc[window] += branch
        pre_acc[window] += grad_normed

    @pl.when(group == pl.num_programs(0) - 1)
    def _():
        back_ref[0, 0] = branch_acc[window].astype(BF16)
        total = pre_acc[window]
        normal = normed_ref[window].astype(F32)
        mean = jnp.mean(total, axis=-1, keepdims=True)
        along = jnp.mean(total * normal, axis=-1, keepdims=True)
        pre = inv_ref[window][:, :1] * (total - mean - normal * along)
        back_ref[0, 1] = pre.astype(BF16)

    turned = [grad_q_t.astype(BF16), grad_k.T.astype(BF16), grad_v.T.astype(BF16)]
    grad_w = nn(jnp.concatenate(turned, axis=0), normed).reshape(3, wide, grads.shape[1])
    grad_p = nn(att_t.astype(BF16), grads).T
    kind = gw_ref.dtype
    if carried:
        first_w, first_p = grad_w + gw_in[...], grad_p + gp_in[...]
    else:
        first_w, first_p = grad_w, grad_p
    if last:
        gw_ref[...] = first_w.astype(kind)
        gp_ref[...] = first_p.astype(kind)
        return

    @pl.when(window == 0)
    def _():
        gw_ref[...] = first_w
        gp_ref[...] = first_p

    @pl.when(window > 0)
    def _():
        gw_ref[...] += grad_w
        gp_ref[...] += grad_p


def attention(normed, inv, gs, regions, w_qkv, w_proj, carry=(), last=False):
    windows, count, width = normed.shape
    assert not last or windows == 1
    wide = GROUP * LANES
    number = width // wide
    whole = lambda *shape: pl.BlockSpec(shape, lambda p, w: (0,) * len(shape))
    rows3 = pl.BlockSpec((3, wide, width), lambda p, w: (0, p, 0))
    cols1 = pl.BlockSpec((width, wide), lambda p, w: (0, p))
    kind = BF16 if last else F32
    return pl.pallas_call(
        functools.partial(attention_kernel, carried=bool(carry), last=last),
        grid=(number, windows),
        in_specs=[
            whole(windows, count, width),
            whole(windows, count, LANES),
            whole(windows, count, width),
            whole(windows, 1, count),
            rows3,
            cols1,
        ]
        + ([rows3, cols1] if carry else []),
        out_specs=[
            pl.BlockSpec(
                (1, 2, count, width), lambda p, w: (jnp.where(p == number - 1, w, 0), 0, 0, 0)
            ),
            rows3,
            cols1,
        ],
        out_shape=(
            jax.ShapeDtypeStruct((windows, 2, count, width), BF16),
            jax.ShapeDtypeStruct((3, width, width), kind),
            jax.ShapeDtypeStruct((width, width), kind),
        ),
        scratch_shapes=[pltpu.VMEM((windows, count, width), F32)] * 2,
        input_output_aliases={6: 1, 7: 2} if carry and not last else {},
        cost_estimate=pl.CostEstimate(
            flops=windows * count * width * (20 * width + 12 * count), transcendentals=0,
            bytes_accessed=windows * count * width * 12),
    )(normed, inv, gs, regions[:, None, :], w_qkv, w_proj, *carry)


def send_kernel(below, second, east, f_ref, g_ref, out_ref, gout_ref, east0, east1, low_ref,
                corner_ref):
    n = f_ref.shape[0]

    @pl.loop(0, n, unroll=3)
    def _(p):
        for i in range(2):
            tokens = east[0, i, p].astype(F32)
            east0[i, p] = unpick(tokens, tokens)[1].astype(BF16)

    @pl.when(pl.program_id(0) == 0)
    def _():
        @pl.loop(0, n, unroll=3)
        def _(p):
            for i, (x, o) in enumerate(((f_ref, out_ref), (g_ref, gout_ref))):
                add, strip = unpick(below[0, i, p].astype(F32), second[0, i, p].astype(F32))
                o[p] = (x[p].astype(F32) + add).astype(BF16)
                east1[i, p] = strip.astype(BF16)

    @pl.when(pl.program_id(0) == 1)
    def _():
        @pl.loop(0, n, unroll=3)
        def _(p):
            for i in range(2):
                add, strip = unpick(below[0, i, p].astype(F32), second[0, i, p].astype(F32))
                low_ref[i, p] = add.astype(BF16)
                corner_ref[i, p] = strip.astype(BF16)


def send(below, second, fields, grads, skip):
    pairs, _, width = fields.shape
    last = pairs // skip - 1
    own = pl.BlockSpec((skip, 48, width), lambda s: (last, 0, 0))
    half = lambda at: pl.BlockSpec((1, 2, skip, 3 * SUB, width), lambda s: (at, 0, s, 0, 0))
    whole = lambda *shape: pl.BlockSpec(shape, lambda s: (0,) * len(shape))
    strips = [(2, skip, 16, width), (2, skip, 48, width), (2, skip, 16, width)]
    outs = [(pairs, 48, width)] * 2 + [(2, 2 * skip, 16, width)] + strips
    return pl.pallas_call(
        send_kernel,
        grid=(2,),
        in_specs=[half(0), half(1), half(0), own, own],
        out_specs=[own, own, pl.BlockSpec((2, skip, 16, width), lambda s: (0, s, 0, 0))]
        + [whole(*shape) for shape in strips],
        out_shape=tuple(jax.ShapeDtypeStruct(shape, BF16) for shape in outs),
        name="send",
    )(below, second, second, fields, grads)


def finish_kernel(first, second, f_ref, g_ref, any0, any1, out_ref, gout_ref):
    @pl.loop(0, f_ref.shape[0], unroll=3)
    def _(p):
        for i, (x, o) in enumerate(((f_ref, out_ref), (g_ref, gout_ref))):
            add, _ = unpick(first[0, i, p].astype(F32), second[0, i, p].astype(F32))
            o[p] = (x[p].astype(F32) + add).astype(BF16)


def finish(first, second, fields, grads, skip, out, gout):
    pairs, _, width = fields.shape
    own = pl.BlockSpec((skip, 48, width), lambda s: (s + 1, 0, 0))
    anyw = pl.BlockSpec(memory_space=pl.ANY)
    half = pl.BlockSpec((1, 2, skip, 3 * SUB, width), lambda s: (0, 0, s, 0, 0))
    return pl.pallas_call(
        finish_kernel,
        grid=(2,),
        in_specs=[half, half, own, own, anyw, anyw],
        out_specs=[own, own],
        out_shape=(jax.ShapeDtypeStruct((pairs, 48, width), BF16),) * 2,
        input_output_aliases={4: 0, 5: 1},
        name="finish",
    )(first, second, fields, grads, out, gout)


def edge_kernel(f_ref, o_ref, r_ref, g_ref, q_ref, out_ref, gout_ref):
    s = lax.broadcasted_iota(jnp.int32, f_ref.shape, 1)
    for i, (f, o, out) in enumerate(((f_ref, o_ref, out_ref), (g_ref, q_ref, gout_ref))):
        total = f[...].astype(F32) + r_ref[i].astype(F32)
        out[...] = jnp.where(s < HALF, total, o[...].astype(F32)).astype(BF16)


def edge(fields, out, back, grads, gout, skip, first):
    _, _, width = fields.shape
    n = back.shape[1] // skip
    at = pl.BlockSpec((skip, SUB, width), lambda i: (i + first, 0, 0))
    strip = pl.BlockSpec((2, skip, SUB, width), lambda i: (0, i, 0, 0))
    return pl.pallas_call(
        edge_kernel,
        grid=(n,),
        in_specs=[at, at, strip, at, at],
        out_specs=[at, at],
        out_shape=(jax.ShapeDtypeStruct(out.shape, BF16),) * 2,
        input_output_aliases={1: 0, 4: 1},
        name="edge",
    )(fields, out, back, grads, gout)


def rim_kernel(f_ref, low_ref, c_ref, g_ref, out_any, gout_any, out_ref, gout_ref):
    for i, (f, out) in enumerate(((f_ref, out_ref), (g_ref, gout_ref))):
        back = low_ref[i].astype(F32)
        corner = c_ref[i].astype(F32)
        s = lax.broadcasted_iota(jnp.int32, corner.shape, 1)
        head = jnp.where(s < HALF, corner, back[:, :SUB])
        back = jnp.concatenate([head, back[:, SUB:]], axis=1)
        out[...] = (f[...].astype(F32) + back).astype(BF16)


def rim(fields, low, corner, grads, out, gout):
    _, skip, cols, width = low.shape
    at = pl.BlockSpec((skip, cols, width), lambda i: (0, 0, 0))
    whole = lambda *shape: pl.BlockSpec(shape, lambda i: (0,) * len(shape))
    anyw = pl.BlockSpec(memory_space=pl.ANY)
    return pl.pallas_call(
        rim_kernel,
        grid=(1,),
        in_specs=[at, whole(2, skip, cols, width), whole(2, skip, SUB, width), at, anyw, anyw],
        out_specs=[at, at],
        out_shape=(jax.ShapeDtypeStruct(out.shape, BF16),) * 2,
        input_output_aliases={4: 0, 5: 1},
        name="rim",
    )(fields, low, corner, grads, out, gout)


def linear(lon, lat, lats):
    return lon * lats + lat


def shift_by(block, step_lon, step_lat):
    lons, lats = lax.axis_size("lon"), lax.axis_size("lat")
    route = [
        (linear((i + step_lon) % lons, (j + step_lat) % lats, lats), linear(i, j, lats))
        for i in range(lons)
        for j in range(lats)
    ]
    return lax.ppermute(block, AXES, route)


def stages():
    lons, lats = lax.axis_size("lon"), lax.axis_size("lat")
    lat_bits = [1 << i for i in range(lats.bit_length() - 1)]
    lon_bits = [lats << i for i in range(lons.bit_length() - 1)]
    assert lats == 1 << len(lat_bits) and lons == 1 << len(lon_bits)
    far = lon_bits[1:]
    groups = [lat_bits[i : i + 2] for i in range(0, len(lat_bits), 2)]
    groups += [far[i : i + 2] for i in range(0, len(far), 2)]
    groups += [lon_bits[:1]]
    return groups, sorted(lat_bits + lon_bits)[::-1]


def swap(block, bit):
    total = lax.axis_size("lon") * lax.axis_size("lat")
    return lax.ppermute(block, AXES, [(i, i ^ bit) for i in range(total)])


def join(mine, other, bit, bits, place):
    high = (place & bit) != 0
    axis = bits.index(bit)
    return jnp.where(
        high,
        jnp.concatenate([other, mine], axis=axis),
        jnp.concatenate([mine, other], axis=axis),
    )


def gather_stage(held, group, bits, place):
    if len(group) == 1:
        return join(held, swap(held, group[0]), group[0], bits, place)
    b1, b2 = group
    o1, o2, o3 = swap(held, b1), swap(held, b2), swap(held, b1 | b2)
    return join(join(held, o1, b1, bits, place), join(o2, o3, b1, bits, place), b2, bits, place)


def part_of(held, bit, bits, index):
    return lax.dynamic_index_in_dim(held, index, bits.index(bit), keepdims=True)


def scatter_stage(held, group, bits, place):
    here = [jnp.where((place & bit) != 0, 1, 0) for bit in group]
    total = held
    for bit, i in zip(group, here):
        total = part_of(total, bit, bits, i)
    total = total.astype(F32)
    for flips in range(1, 1 << len(group)):
        send, mask = held, 0
        for k, (bit, i) in enumerate(zip(group, here)):
            flip = (flips >> k) & 1
            send = part_of(send, bit, bits, 1 - i if flip else i)
            mask |= bit * flip
        total = total + swap(send.astype(BF16), mask).astype(F32)
    return total


def lines_of(grid):
    rows, cols, levels, width = grid.shape
    return grid.transpose(0, 2, 1, 3).reshape(rows * levels, cols, width)


def grid_of(lines, levels):
    count, cols, width = lines.shape
    return lines.reshape(count // levels, levels, cols, width).transpose(0, 2, 1, 3)


def paired(lines):
    *lead, count, cols, width = lines.shape
    return lines.reshape(*lead, count // 2, 2 * cols, width)


def unpaired(pairs):
    *lead, count, cols, width = pairs.shape
    return pairs.reshape(*lead, count * 2, cols // 2, width)


def block(fields, region_ids, w_qkv, w_proj, grad_output):
    rows, cols, levels, width = fields.shape
    skip = HALF * levels // 2
    devices = lax.axis_size("lon") * lax.axis_size("lat")
    factor = float(rows * cols * levels * devices) ** (-0.5)
    place = lax.axis_index(AXES)
    groups, bits = stages()
    share = w_qkv.shape[0]
    f_lines, g_lines = lines_of(fields), lines_of(grad_output)
    f_pairs, g_pairs = paired(f_lines), paired(g_lines)
    held = jnp.concatenate([w_qkv, w_proj], axis=0)
    held = held.reshape((1,) * len(bits) + held.shape)
    for group in groups[:-1]:
        held = gather_stage(held, group, bits, place)
    bit = groups[-1][0]
    other = swap(held, bit)
    w3 = join(held[..., :share, :], other[..., :share, :], bit, bits, place).reshape(3, width, width)
    p_all = join(held[..., share:, :], other[..., share:, :], bit, bits, place).reshape(width, width)
    low, corner, east = pack(f_lines, g_lines, 2 * skip)
    low = shift_by(low, 0, 1)
    east = shift_by(east, 1, 0)
    corner = shift_by(corner, 1, 1)
    low, east, corner = paired(low), paired(east), paired(corner)
    regions = token_regions(region_ids, levels)
    n00, i00, g00 = assemble_own(f_pairs, g_pairs, skip)
    n10, i10, g10 = assemble_below(f_pairs, g_pairs, low, skip)
    b10, *carry = attention(n10, i10, g10, regions[1, :1], w3, p_all)
    n1, i1, g1 = assemble_second(f_pairs, g_pairs, east, low, corner, skip)
    b1, *carry = attention(n1, i1, g1, regions[:, 1], w3, p_all, carry)
    b10, b1 = [x.reshape(-1, 2, 2 * skip, 3 * SUB, width) for x in (b10, b1)]
    out, gout, r_east0, r_east1, r_low, r_corner = send(b10, b1, f_pairs, g_pairs, skip)
    r_low = shift_by(unpaired(r_low), 0, -1)
    r_corner = shift_by(unpaired(r_corner), -1, -1)
    r_east1 = shift_by(unpaired(r_east1), -1, 0)
    r_east0 = shift_by(unpaired(r_east0), -1, 0)
    b00, grad_w, grad_p = attention(n00, i00, g00, regions[0, :1], w3, p_all, carry, True)
    b00 = b00.reshape(-1, 2, 2 * skip, 3 * SUB, width)
    grads = jnp.concatenate(
        [grad_w.reshape(devices, -1, width), grad_p.reshape(devices, -1, width)], axis=1
    )
    grads = grads.reshape((2,) * len(bits) + grads.shape[1:])
    for group in groups[::-1]:
        grads = scatter_stage(grads, group, bits, place)
    grads = grads.reshape(-1, width) * factor
    out, gout = finish(b00, b1, f_pairs, g_pairs, skip, out, gout)
    out, gout = unpaired(out), unpaired(gout)
    out, gout = rim(f_lines, r_low, r_corner, g_lines, out, gout)
    out, gout = edge(f_lines, out, r_east1, g_lines, gout, 2 * skip, rows * levels // (2 * skip) - 1)
    out, gout = edge(f_lines, out, r_east0, g_lines, gout, 2 * skip, 1)
    return (grid_of(out, levels), grid_of(gout, levels), grads[:share], grads[share:])


def solution(mesh):
    return jax.shard_map(
        block,
        mesh=mesh,
        in_specs=(
            P("lat", "lon", None, None),
            P("lat"),
            P(AXES, None),
            P(AXES, None),
            P("lat", "lon", None, None),
        ),
        out_specs=(
            P("lat", "lon", None, None),
            P("lat", "lon", None, None),
            P(AXES, None),
            P(AXES, None),
        ),
        check_vma=False,
    )
```

```python
import functools

import jax
import jax.numpy as jnp
from jax import lax
from jax.experimental import pallas as pl
from jax.experimental.pallas import tpu as pltpu
from jax.sharding import PartitionSpec as P


HEAD = 64
WIN = 12
HALF = WIN // 2
EPSILON = 1e-05
AXES = ("lon", "lat")
LANES = 128
SUB = 8


F32 = jnp.float32
BF16 = jnp.bfloat16


def nt(a, b):
    return lax.dot_general(a, b, (((1,), (1,)), ((), ())), preferred_element_type=F32)


def nn(a, b):
    return lax.dot_general(a, b, (((1,), (0,)), ((), ())), preferred_element_type=F32)


GROUP = 2


def sub_index(width):
    return lax.broadcasted_iota(jnp.int32, (SUB, width), 0)


def pick_first(own):
    s = sub_index(own.shape[1])
    t0a, t1a, t2a, t0b, t1b, t2b = [own[8 * i : 8 * i + 8] for i in range(6)]
    mixed = jnp.where(
        s < 2,
        t2a,
        jnp.where(s < 4, pltpu.roll(t2b, 2, 0), jnp.where(s < 6, pltpu.roll(t0b, 6, 0), t0a)),
    )
    return jnp.concatenate([t1a, t1b, mixed], axis=0)


def pick_second(own, strip):
    s = sub_index(own.shape[1])
    t2a, t2b = own[16:24], own[40:48]
    ha, hb = strip[:8], strip[8:]
    n1 = jnp.where(s < 2, ha, t2a)
    n2 = jnp.where(s < 2, hb, t2b)
    n3 = jnp.where((s >= 2) & (s < 6), ha, pltpu.roll(hb, 4, 0))
    return jnp.concatenate([n1, n2, n3], axis=0)


def unpick(first, second):
    s = sub_index(first.shape[1])
    t1a, t1b, mixed = first[:8], first[8:16], first[16:]
    n1, n2, n3 = second[:8], second[8:16], second[16:]
    zero = jnp.zeros_like(mixed)
    t0a = jnp.where(s >= 6, mixed, zero)
    t0b = jnp.where(s >= 6, pltpu.roll(mixed, 2, 0), zero)
    t2a = jnp.where(s < 2, mixed, n1)
    t2b = jnp.where(s < 2, pltpu.roll(mixed, 6, 0), n2)
    ha = jnp.where(s < 2, n1, n3)
    hb = jnp.where(s < 2, n2, pltpu.roll(n3, 4, 0))
    own = jnp.concatenate([t0a, t1a, t2a, t0b, t1b, t2b], axis=0)
    return own, jnp.concatenate([ha, hb], axis=0)


def token_regions(region_ids, levels):
    lines = jnp.repeat(region_ids, levels)
    pairs = lines.reshape(-1, 2)
    s = jnp.arange(3 * SUB)
    inner = s % SUB
    line0 = jnp.where(s < 8, 0, jnp.where(s < 16, 1, jnp.where((inner < 2) | (inner >= 6), 0, 1)))
    line1 = jnp.where(s < 8, 0, jnp.where(s < 16, 1, jnp.where((inner >= 2) & (inner < 6), 0, 1)))
    a, b = pairs[:, :1], pairs[:, 1:]
    both = jnp.stack([jnp.where(line0 == 0, a, b), jnp.where(line1 == 0, a, b)])
    per_band = WIN * levels // 2
    bands = pairs.shape[0] // per_band
    return both.reshape(2, bands, per_band * 3 * SUB).transpose(1, 0, 2)


def pack_kernel(f_ref, f_first, g_ref, g_first, low_ref, corner_ref, east_ref):
    n = low_ref.shape[1]
    for i, (x, first) in enumerate(((f_ref, f_first), (g_ref, g_first))):
        low_ref[i] = x[...]
        corner_ref[i] = first[:n]
        east_ref[i] = first[n:]


def pack(f_lines, g_lines, n):
    lines, cols, width = f_lines.shape
    low = pl.BlockSpec((n, cols, width), lambda i: (0, 0, 0))
    first = pl.BlockSpec((lines, SUB, width), lambda i: (0, 0, 0))
    shapes = [(2, n, cols, width), (2, n, SUB, width), (2, lines - n, SUB, width)]
    return pl.pallas_call(
        pack_kernel,
        grid=(1,),
        in_specs=[low, first, low, first],
        out_specs=[pl.BlockSpec(shape, lambda i: (0,) * 4) for shape in shapes],
        out_shape=tuple(jax.ShapeDtypeStruct(shape, BF16) for shape in shapes),
        name="pack",
    )(f_lines, f_lines, g_lines, g_lines)


def norm(block):
    centre = block - jnp.mean(block, axis=-1, keepdims=True)
    inverse = lax.rsqrt(jnp.mean(centre * centre, axis=-1, keepdims=True) + EPSILON)
    return (centre * inverse).astype(BF16), inverse


def put(at, p, block, grads, normed_ref, inv_ref, gs_ref):
    normed, inverse = norm(block)
    normed_ref[at, p] = normed
    inv_ref[at, p] = jnp.broadcast_to(inverse, (3 * SUB, LANES))
    gs_ref[at, p] = grads.astype(BF16)


def assemble_own_kernel(f_ref, g_ref, *outs):
    @pl.loop(0, f_ref.shape[0], unroll=9)
    def _(p):
        put(0, p, pick_first(f_ref[p].astype(F32)), pick_first(g_ref[p].astype(F32)), *outs)


def assemble_below_kernel(f_ref, g_ref, low_ref, *outs):
    @pl.when(pl.program_id(0) == 0)
    def _():
        @pl.loop(0, f_ref.shape[0], unroll=9)
        def _(p):
            put(0, p, pick_first(f_ref[p].astype(F32)), pick_first(g_ref[p].astype(F32)), *outs)

    @pl.when(pl.program_id(0) == 1)
    def _():
        @pl.loop(0, f_ref.shape[0], unroll=9)
        def _(p):
            put(0, p, pick_first(low_ref[0, p].astype(F32)), pick_first(low_ref[1, p].astype(F32)), *outs)


def assemble_second_kernel(f_ref, g_ref, east_ref, low_ref, corner_ref, *outs):
    last = pl.num_programs(0) - 1

    @pl.when(pl.program_id(0) < last)
    def _():
        @pl.loop(0, f_ref.shape[0], unroll=9)
        def _(p):
            put(
                0,
                p,
                pick_second(f_ref[p].astype(F32), east_ref[0, p].astype(F32)),
                pick_second(g_ref[p].astype(F32), east_ref[1, p].astype(F32)),
                *outs,
            )

    @pl.when(pl.program_id(0) == last)
    def _():
        @pl.loop(0, f_ref.shape[0], unroll=9)
        def _(p):
            put(
                0,
                p,
                pick_second(low_ref[0, p].astype(F32), corner_ref[0, p].astype(F32)),
                pick_second(low_ref[1, p].astype(F32), corner_ref[1, p].astype(F32)),
                *outs,
            )


def assembled(kernel, windows, skip, width, specs, args):
    shape = (windows, 2 * skip, 3 * SUB)
    out = lambda w: pl.BlockSpec((1, skip, 3 * SUB, w), lambda s: (s // 2, s % 2, 0, 0))
    outs = pl.pallas_call(
        kernel,
        grid=(2 * windows,),
        in_specs=specs,
        out_specs=[out(width), out(LANES), out(width)],
        out_shape=(
            jax.ShapeDtypeStruct(shape + (width,), BF16),
            jax.ShapeDtypeStruct(shape + (LANES,), F32),
            jax.ShapeDtypeStruct(shape + (width,), BF16),
        ),
        cost_estimate=pl.CostEstimate(
            flops=windows * skip * 3 * SUB * width * 100, transcendentals=0,
            bytes_accessed=windows * skip * 3 * SUB * width * 16),
    )(*args)
    count = 2 * skip * 3 * SUB
    return [x.reshape(windows, count, x.shape[-1]) for x in outs]


def assemble_own(fields, grads, skip):
    width = fields.shape[2]
    own = pl.BlockSpec((skip, 48, width), lambda s: (s + 1, 0, 0))
    return assembled(assemble_own_kernel, 1, skip, width, [own, own], (fields, grads))


def assemble_below(fields, grads, low, skip):
    width = fields.shape[2]
    last = fields.shape[0] // skip - 1
    own = pl.BlockSpec((skip, 48, width), lambda s: (last, 0, 0))
    below = pl.BlockSpec((2, skip, 48, width), lambda s: (0, 0, 0, 0))
    return assembled(assemble_below_kernel, 1, skip, width, [own, own, below], (fields, grads, low))


def assemble_second(fields, grads, east, low, corner, skip):
    width = fields.shape[2]
    n = fields.shape[0] // skip - 1
    own = pl.BlockSpec((skip, 48, width), lambda s: (jnp.minimum(s + 1, n), 0, 0))
    strip = pl.BlockSpec((2, skip, 16, width), lambda s: (0, jnp.minimum(s, n - 1), 0, 0))
    below = pl.BlockSpec((2, skip, 48, width), lambda s: (0, 0, 0, 0))
    diagonal = pl.BlockSpec((2, skip, 16, width), lambda s: (0, 0, 0, 0))
    return assembled(
        assemble_second_kernel, (n + 1) // 2, skip, width, [own, own, strip, below, diagonal],
        (fields, grads, east, low, corner),
    )


def attention_kernel(*refs, carried, last):
    normed_ref, inv_ref, gs_ref, reg_ref, w_ref, wp_ref = refs[:6]
    refs = refs[6:]
    gw_in = gp_in = None
    if carried:
        gw_in, gp_in = refs[:2]
        refs = refs[2:]
    back_ref, gw_ref, gp_ref, branch_acc, pre_acc = refs
    group = pl.program_id(0)
    window = pl.program_id(1)
    scale = HEAD ** (-0.5)
    normed = normed_ref[window]
    grads = gs_ref[window]
    count = normed.shape[0]
    wide = GROUP * LANES
    weights = w_ref[...].reshape(3 * wide, w_ref.shape[2])
    qkv = nt(normed, weights).astype(BF16)
    queries, all_keys, all_values = [qkv[:, wide * i : wide * (i + 1)] for i in range(3)]
    queries = queries * jnp.asarray(scale, BF16)
    grad_att_all = nn(grads, wp_ref[...]).astype(BF16)
    all_keys_t = all_keys.astype(F32).T.astype(BF16) * jnp.asarray(scale, BF16)
    all_values_t = all_values.astype(F32).T.astype(BF16)
    region = reg_ref[window]
    region_t = jnp.broadcast_to(region, (LANES, count)).T
    spread = jnp.concatenate([region_t] * -(-count // LANES), axis=1)[:, :count]
    allowed = spread == region
    lane = lax.broadcasted_iota(jnp.int32, (count, LANES), 1)
    zero = jnp.zeros((), BF16)
    heads = GROUP * LANES // HEAD
    pairs = LANES // HEAD

    def inputs(h):
        pair, k = divmod(h, pairs)
        cols = slice(pair * LANES, (pair + 1) * LANES)
        mine = (lane >= k * HEAD) & (lane < (k + 1) * HEAD)
        return cols, lambda x: jnp.where(mine, x[:, cols], zero)

    def products(h):
        cols, only = inputs(h)
        scores = nt(only(all_keys), queries[:, cols])
        return jnp.where(allowed, scores, -1e30), nt(only(all_values), grad_att_all[:, cols])

    def softmax(scores, grad_probs):
        peak = jnp.max(scores, axis=0, keepdims=True)
        expo = jnp.exp(scores - peak)
        ratio = 1.0 / jnp.sum(expo, axis=0, keepdims=True)
        rounded = (expo * ratio).astype(BF16)
        inner = jnp.sum(grad_probs * expo, axis=0, keepdims=True) * ratio
        return rounded, (expo * (grad_probs - inner) * ratio).astype(BF16)

    def gradients(h, rounded, grad_scores):
        _, only = inputs(h)
        rows = slice(h * HEAD, (h + 1) * HEAD)
        return (
            nn(all_values_t[rows], rounded),
            nn(all_keys_t[rows], grad_scores),
            nn(grad_scores, only(queries)),
            nn(rounded, only(grad_att_all)),
        )

    def joined(k, first, number):
        return jnp.concatenate([d[k] for d in done[first * pairs : (first + number) * pairs]], axis=0)

    def att_rows(first, number):
        return joined(0, first, number).T.astype(BF16)

    def back_to_rows(first, number):
        return joined(1, first, number).T.astype(BF16)

    def key_and_value(first, number, turned=False):
        out = []
        for k in (2, 3):
            both = [
                sum(d[k] for d in done[p * pairs : (p + 1) * pairs]) for p in range(first, first + number)
            ]
            if turned:
                out.append(jnp.concatenate([x.T.astype(BF16) for x in both], axis=0))
            else:
                out.append(jnp.concatenate([x.astype(BF16) for x in both], axis=1))
        return out

    def sums(first, number):
        turned = [joined(1, first, number).astype(BF16), *key_and_value(first, number, True)]
        grad_w = nn(jnp.concatenate(turned, axis=0), normed)
        grad_w = grad_w.reshape(3, number * LANES, grad_w.shape[1])
        return grad_w, nn(joined(0, first, number).astype(BF16), grads).T, first

    ahead, weights_of, done = {0: products(0)}, {}, []
    parts = [(0, GROUP)]
    early = {}
    for h in range(heads + 1):
        if h + 1 < heads:
            ahead[h + 1] = products(h + 1)
        if h < heads:
            weights_of[h] = softmax(*ahead.pop(h))
        if h > 0:
            done.append(gradients(h - 1, *weights_of.pop(h - 1)))
    att = att_rows(0, GROUP)
    grad_qkv = jnp.concatenate([back_to_rows(0, GROUP), *key_and_value(0, GROUP)], axis=1)
    branch = nt(att, wp_ref[...])
    grad_normed = nn(grad_qkv, weights)
    started = group > 0
    branch += jnp.where(started, branch_acc[window], 0.0)
    grad_normed += jnp.where(started, pre_acc[window], 0.0)
    branch_acc[window] = branch
    pre_acc[window] = grad_normed
    back_ref[0, 0] = branch.astype(BF16)
    normal = normed.astype(F32)
    mean = jnp.mean(grad_normed, axis=-1, keepdims=True)
    along = jnp.mean(grad_normed * normal, axis=-1, keepdims=True)
    pre = inv_ref[window][:, :1] * (grad_normed - mean - normal * along)
    back_ref[0, 1] = pre.astype(BF16)
    opening = window == 0
    kind = gw_ref.dtype
    for pairs_of in parts:
        grad_w, grad_p, at = sums(*pairs_of) if pairs_of not in early else early[pairs_of]
        cols = pl.ds(at * LANES, grad_p.shape[1])
        for ref, mine, carry, where in (
            (gw_ref, grad_w, gw_in, (slice(None), cols)),
            (gp_ref, grad_p, gp_in, (slice(None), cols)),
        ):
            if last:
                ref[where] = (mine + carry[where] if carried else mine).astype(kind)
            else:
                base = carry[where] if carried else 0.0
                ref[where] = mine + jnp.where(opening, base, ref[where])


def attention(normed, inv, gs, regions, w_qkv, w_proj, carry=(), last=False):
    windows, count, width = normed.shape
    assert not last or windows == 1
    wide = GROUP * LANES
    number = width // wide
    whole = lambda *shape: pl.BlockSpec(shape, lambda p, w: (0,) * len(shape))
    rows3 = pl.BlockSpec((3, wide, width), lambda p, w: (0, p, 0))
    cols1 = pl.BlockSpec((width, wide), lambda p, w: (0, p))
    kind = BF16 if last else F32
    return pl.pallas_call(
        functools.partial(attention_kernel, carried=bool(carry), last=last),
        grid=(number, windows),
        in_specs=[
            whole(windows, count, width),
            whole(windows, count, LANES),
            whole(windows, count, width),
            whole(windows, 1, count),
            rows3,
            cols1,
        ]
        + ([rows3, cols1] if carry else []),
        out_specs=[
            pl.BlockSpec(
                (1, 2, count, width), lambda p, w: (jnp.where(p == number - 1, w, 0), 0, 0, 0)
            ),
            rows3,
            cols1,
        ],
        out_shape=(
            jax.ShapeDtypeStruct((windows, 2, count, width), BF16),
            jax.ShapeDtypeStruct((3, width, width), kind),
            jax.ShapeDtypeStruct((width, width), kind),
        ),
        scratch_shapes=[pltpu.VMEM((windows, count, width), F32)] * 2,
        input_output_aliases={6: 1, 7: 2} if carry and not last else {},
        cost_estimate=pl.CostEstimate(
            flops=windows * count * width * (20 * width + 12 * count), transcendentals=0,
            bytes_accessed=windows * count * width * 12),
    )(normed, inv, gs, regions[:, None, :], w_qkv, w_proj, *carry)


def send_kernel(below, second, east, f_ref, g_ref, out_ref, gout_ref, east0, east1, low_ref,
                corner_ref):
    n = f_ref.shape[0]

    @pl.loop(0, n, unroll=3)
    def _(p):
        for i in range(2):
            tokens = east[0, i, p].astype(F32)
            east0[i, p] = unpick(tokens, tokens)[1].astype(BF16)

    @pl.when(pl.program_id(0) == 0)
    def _():
        @pl.loop(0, n, unroll=3)
        def _(p):
            for i, (x, o) in enumerate(((f_ref, out_ref), (g_ref, gout_ref))):
                add, strip = unpick(below[0, i, p].astype(F32), second[0, i, p].astype(F32))
                o[p] = (x[p].astype(F32) + add).astype(BF16)
                east1[i, p] = strip.astype(BF16)

    @pl.when(pl.program_id(0) == 1)
    def _():
        @pl.loop(0, n, unroll=3)
        def _(p):
            for i in range(2):
                add, strip = unpick(below[0, i, p].astype(F32), second[0, i, p].astype(F32))
                low_ref[i, p] = add.astype(BF16)
                corner_ref[i, p] = strip.astype(BF16)


def send(below, second, fields, grads, skip):
    pairs, _, width = fields.shape
    last = pairs // skip - 1
    own = pl.BlockSpec((skip, 48, width), lambda s: (last, 0, 0))
    half = lambda at: pl.BlockSpec((1, 2, skip, 3 * SUB, width), lambda s: (at, 0, s, 0, 0))
    whole = lambda *shape: pl.BlockSpec(shape, lambda s: (0,) * len(shape))
    strips = [(2, skip, 16, width), (2, skip, 48, width), (2, skip, 16, width)]
    outs = [(pairs, 48, width)] * 2 + [(2, 2 * skip, 16, width)] + strips
    return pl.pallas_call(
        send_kernel,
        grid=(2,),
        in_specs=[half(0), half(1), half(0), own, own],
        out_specs=[own, own, pl.BlockSpec((2, skip, 16, width), lambda s: (0, s, 0, 0))]
        + [whole(*shape) for shape in strips],
        out_shape=tuple(jax.ShapeDtypeStruct(shape, BF16) for shape in outs),
        name="send",
    )(below, second, second, fields, grads)


def finish_kernel(first, second, f_ref, g_ref, any0, any1, out_ref, gout_ref):
    @pl.loop(0, f_ref.shape[0], unroll=3)
    def _(p):
        for i, (x, o) in enumerate(((f_ref, out_ref), (g_ref, gout_ref))):
            add, _ = unpick(first[0, i, p].astype(F32), second[0, i, p].astype(F32))
            o[p] = (x[p].astype(F32) + add).astype(BF16)


def finish(first, second, fields, grads, skip, out, gout):
    pairs, _, width = fields.shape
    own = pl.BlockSpec((skip, 48, width), lambda s: (s + 1, 0, 0))
    anyw = pl.BlockSpec(memory_space=pl.ANY)
    half = pl.BlockSpec((1, 2, skip, 3 * SUB, width), lambda s: (0, 0, s, 0, 0))
    return pl.pallas_call(
        finish_kernel,
        grid=(2,),
        in_specs=[half, half, own, own, anyw, anyw],
        out_specs=[own, own],
        out_shape=(jax.ShapeDtypeStruct((pairs, 48, width), BF16),) * 2,
        input_output_aliases={4: 0, 5: 1},
        name="finish",
    )(first, second, fields, grads, out, gout)


def edge_kernel(f_ref, o_ref, r_ref, g_ref, q_ref, out_ref, gout_ref):
    s = lax.broadcasted_iota(jnp.int32, f_ref.shape, 1)
    for i, (f, o, out) in enumerate(((f_ref, o_ref, out_ref), (g_ref, q_ref, gout_ref))):
        total = f[...].astype(F32) + r_ref[i].astype(F32)
        out[...] = jnp.where(s < HALF, total, o[...].astype(F32)).astype(BF16)


def edge(fields, out, back, grads, gout, skip, first):
    _, _, width = fields.shape
    n = back.shape[1] // skip
    at = pl.BlockSpec((skip, SUB, width), lambda i: (i + first, 0, 0))
    strip = pl.BlockSpec((2, skip, SUB, width), lambda i: (0, i, 0, 0))
    return pl.pallas_call(
        edge_kernel,
        grid=(n,),
        in_specs=[at, at, strip, at, at],
        out_specs=[at, at],
        out_shape=(jax.ShapeDtypeStruct(out.shape, BF16),) * 2,
        input_output_aliases={1: 0, 4: 1},
        name="edge",
    )(fields, out, back, grads, gout)


def rim_kernel(f_ref, low_ref, c_ref, g_ref, out_any, gout_any, out_ref, gout_ref):
    for i, (f, out) in enumerate(((f_ref, out_ref), (g_ref, gout_ref))):
        back = low_ref[i].astype(F32)
        corner = c_ref[i].astype(F32)
        s = lax.broadcasted_iota(jnp.int32, corner.shape, 1)
        head = jnp.where(s < HALF, corner, back[:, :SUB])
        back = jnp.concatenate([head, back[:, SUB:]], axis=1)
        out[...] = (f[...].astype(F32) + back).astype(BF16)


def rim(fields, low, corner, grads, out, gout):
    _, skip, cols, width = low.shape
    at = pl.BlockSpec((skip, cols, width), lambda i: (0, 0, 0))
    whole = lambda *shape: pl.BlockSpec(shape, lambda i: (0,) * len(shape))
    anyw = pl.BlockSpec(memory_space=pl.ANY)
    return pl.pallas_call(
        rim_kernel,
        grid=(1,),
        in_specs=[at, whole(2, skip, cols, width), whole(2, skip, SUB, width), at, anyw, anyw],
        out_specs=[at, at],
        out_shape=(jax.ShapeDtypeStruct(out.shape, BF16),) * 2,
        input_output_aliases={4: 0, 5: 1},
        name="rim",
    )(fields, low, corner, grads, out, gout)


def linear(lon, lat, lats):
    return lon * lats + lat


def shift_by(block, step_lon, step_lat):
    lons, lats = lax.axis_size("lon"), lax.axis_size("lat")
    route = [
        (linear((i + step_lon) % lons, (j + step_lat) % lats, lats), linear(i, j, lats))
        for i in range(lons)
        for j in range(lats)
    ]
    return lax.ppermute(block, AXES, route)


def stages():
    lons, lats = lax.axis_size("lon"), lax.axis_size("lat")
    lat_bits = [1 << i for i in range(lats.bit_length() - 1)]
    lon_bits = [lats << i for i in range(lons.bit_length() - 1)]
    assert lats == 1 << len(lat_bits) and lons == 1 << len(lon_bits)
    far = lon_bits[1:]
    groups = [lat_bits[i : i + 2] for i in range(0, len(lat_bits), 2)]
    groups += [far[i : i + 2] for i in range(0, len(far), 2)]
    groups += [lon_bits[:1]]
    return groups, sorted(lat_bits + lon_bits)[::-1]


def swap(block, bit):
    total = lax.axis_size("lon") * lax.axis_size("lat")
    return lax.ppermute(block, AXES, [(i, i ^ bit) for i in range(total)])


def join(mine, other, bit, bits, place):
    high = (place & bit) != 0
    axis = bits.index(bit)
    return jnp.where(
        high,
        jnp.concatenate([other, mine], axis=axis),
        jnp.concatenate([mine, other], axis=axis),
    )


def gather_stage(held, group, bits, place):
    if len(group) == 1:
        return join(held, swap(held, group[0]), group[0], bits, place)
    b1, b2 = group
    o1, o2, o3 = swap(held, b1), swap(held, b2), swap(held, b1 | b2)
    return join(join(held, o1, b1, bits, place), join(o2, o3, b1, bits, place), b2, bits, place)


def part_of(held, bit, bits, index):
    return lax.dynamic_index_in_dim(held, index, bits.index(bit), keepdims=True)


def scatter_stage(held, group, bits, place):
    here = [jnp.where((place & bit) != 0, 1, 0) for bit in group]
    total = held
    for bit, i in zip(group, here):
        total = part_of(total, bit, bits, i)
    total = total.astype(F32)
    for flips in range(1, 1 << len(group)):
        send, mask = held, 0
        for k, (bit, i) in enumerate(zip(group, here)):
            flip = (flips >> k) & 1
            send = part_of(send, bit, bits, 1 - i if flip else i)
            mask |= bit * flip
        total = total + swap(send.astype(BF16), mask).astype(F32)
    return total


def last_join_kernel(place_ref, mine_ref, other_ref, w_ref, p_ref):
    share = w_ref.shape[3]
    for own, ref in ((True, mine_ref), (False, other_ref)):
        at = place_ref[0] if own else 1 - place_ref[0]
        w_ref[:, at] = ref[:, :, :share]
        p_ref[:, at] = ref[:, :, share:]


def last_join(mine, other, place, share):
    far, near, rows, width = mine.shape
    whole = lambda *shape: pl.BlockSpec(shape, lambda i, p: (0,) * len(shape))
    shapes = [(far, 2, near, share, width), (far, 2, near, rows - share, width)]
    return pl.pallas_call(
        last_join_kernel,
        grid_spec=pltpu.PrefetchScalarGridSpec(
            num_scalar_prefetch=1,
            grid=(1,),
            in_specs=[whole(*mine.shape)] * 2,
            out_specs=[whole(*shape) for shape in shapes],
        ),
        out_shape=tuple(jax.ShapeDtypeStruct(shape, BF16) for shape in shapes),
        name="last_join",
    )(place, mine, other)


def lines_of(grid):
    rows, cols, levels, width = grid.shape
    return grid.transpose(0, 2, 1, 3).reshape(rows * levels, cols, width)


def grid_of(lines, levels):
    count, cols, width = lines.shape
    return lines.reshape(count // levels, levels, cols, width).transpose(0, 2, 1, 3)


def paired(lines):
    *lead, count, cols, width = lines.shape
    return lines.reshape(*lead, count // 2, 2 * cols, width)


def unpaired(pairs):
    *lead, count, cols, width = pairs.shape
    return pairs.reshape(*lead, count * 2, cols // 2, width)


def block(fields, region_ids, w_qkv, w_proj, grad_output):
    rows, cols, levels, width = fields.shape
    skip = HALF * levels // 2
    devices = lax.axis_size("lon") * lax.axis_size("lat")
    factor = float(rows * cols * levels * devices) ** (-0.5)
    place = lax.axis_index(AXES)
    groups, bits = stages()
    share = w_qkv.shape[0]
    f_lines, g_lines = lines_of(fields), lines_of(grad_output)
    f_pairs, g_pairs = paired(f_lines), paired(g_lines)
    held = jnp.concatenate([w_qkv, w_proj], axis=0)
    held = held.reshape((1,) * len(bits) + held.shape)
    for group in groups[:-1]:
        held = gather_stage(held, group, bits, place)
    bit = groups[-1][0]
    other = swap(held, bit)
    near = bit
    halves = [x.reshape(-1, near, held.shape[-2], width) for x in (held, other)]
    w3, p_all = last_join(*halves, jnp.where((place & bit) != 0, 1, 0).reshape(1), share)
    w3, p_all = w3.reshape(3, width, width), p_all.reshape(width, width)
    low, corner, east = pack(f_lines, g_lines, 2 * skip)
    low = shift_by(low, 0, 1)
    east = shift_by(east, 1, 0)
    corner = shift_by(corner, 1, 1)
    low, east, corner = paired(low), paired(east), paired(corner)
    regions = token_regions(region_ids, levels)
    n00, i00, g00 = assemble_own(f_pairs, g_pairs, skip)
    n10, i10, g10 = assemble_below(f_pairs, g_pairs, low, skip)
    b10, *carry = attention(n10, i10, g10, regions[1, :1], w3, p_all)
    n1, i1, g1 = assemble_second(f_pairs, g_pairs, east, low, corner, skip)
    b1, *carry = attention(n1, i1, g1, regions[:, 1], w3, p_all, carry)
    b10, b1 = [x.reshape(-1, 2, 2 * skip, 3 * SUB, width) for x in (b10, b1)]
    out, gout, r_east0, r_east1, r_low, r_corner = send(b10, b1, f_pairs, g_pairs, skip)
    r_low = shift_by(unpaired(r_low), 0, -1)
    r_corner = shift_by(unpaired(r_corner), -1, -1)
    r_east1 = shift_by(unpaired(r_east1), -1, 0)
    r_east0 = shift_by(unpaired(r_east0), -1, 0)
    b00, grad_w, grad_p = attention(n00, i00, g00, regions[0, :1], w3, p_all, carry, True)
    b00 = b00.reshape(-1, 2, 2 * skip, 3 * SUB, width)
    grads = jnp.concatenate(
        [grad_w.reshape(devices, -1, width), grad_p.reshape(devices, -1, width)], axis=1
    )
    grads = grads.reshape((2,) * len(bits) + grads.shape[1:])
    for group in groups[::-1]:
        grads = scatter_stage(grads, group, bits, place)
    grads = grads.reshape(-1, width) * factor
    out, gout = finish(b00, b1, f_pairs, g_pairs, skip, out, gout)
    out, gout = unpaired(out), unpaired(gout)
    out, gout = rim(f_lines, r_low, r_corner, g_lines, out, gout)
    out, gout = edge(f_lines, out, r_east1, g_lines, gout, 2 * skip, rows * levels // (2 * skip) - 1)
    out, gout = edge(f_lines, out, r_east0, g_lines, gout, 2 * skip, 1)
    return (grid_of(out, levels), grid_of(gout, levels), grads[:share], grads[share:])


def solution(mesh):
    return jax.shard_map(
        block,
        mesh=mesh,
        in_specs=(
            P("lat", "lon", None, None),
            P("lat"),
            P(AXES, None),
            P(AXES, None),
            P("lat", "lon", None, None),
        ),
        out_specs=(
            P("lat", "lon", None, None),
            P("lat", "lon", None, None),
            P(AXES, None),
            P(AXES, None),
        ),
        check_vma=False,
    )
```

```python
import functools

import jax
import jax.numpy as jnp
from jax import lax
from jax.experimental import pallas as pl
from jax.experimental.pallas import tpu as pltpu
from jax.sharding import PartitionSpec as P


HEAD = 64
WIN = 12
HALF = WIN // 2
EPSILON = 1e-05
AXES = ("lon", "lat")
LANES = 128
SUB = 8


F32 = jnp.float32
BF16 = jnp.bfloat16


def grant(mib):
    return pltpu.CompilerParams(vmem_limit_bytes=mib << 20 if mib else None)


def nt(a, b):
    return lax.dot_general(a, b, (((1,), (1,)), ((), ())), preferred_element_type=F32)


def nn(a, b):
    return lax.dot_general(a, b, (((1,), (0,)), ((), ())), preferred_element_type=F32)


GROUP = 2


def sub_index(width):
    return lax.broadcasted_iota(jnp.int32, (SUB, width), 0)


def pick_first(own):
    s = sub_index(own.shape[1])
    t0a, t1a, t2a, t0b, t1b, t2b = [own[8 * i : 8 * i + 8] for i in range(6)]
    mixed = jnp.where(
        s < 2,
        t2a,
        jnp.where(s < 4, pltpu.roll(t2b, 2, 0), jnp.where(s < 6, pltpu.roll(t0b, 6, 0), t0a)),
    )
    return jnp.concatenate([t1a, t1b, mixed], axis=0)


def pick_second(own, strip):
    s = sub_index(own.shape[1])
    t2a, t2b = own[16:24], own[40:48]
    ha, hb = strip[:8], strip[8:]
    n1 = jnp.where(s < 2, ha, t2a)
    n2 = jnp.where(s < 2, hb, t2b)
    n3 = jnp.where((s >= 2) & (s < 6), ha, pltpu.roll(hb, 4, 0))
    return jnp.concatenate([n1, n2, n3], axis=0)


def unpick(first, second):
    s = sub_index(first.shape[1])
    t1a, t1b, mixed = first[:8], first[8:16], first[16:]
    n1, n2, n3 = second[:8], second[8:16], second[16:]
    zero = jnp.zeros_like(mixed)
    t0a = jnp.where(s >= 6, mixed, zero)
    t0b = jnp.where(s >= 6, pltpu.roll(mixed, 2, 0), zero)
    t2a = jnp.where(s < 2, mixed, n1)
    t2b = jnp.where(s < 2, pltpu.roll(mixed, 6, 0), n2)
    ha = jnp.where(s < 2, n1, n3)
    hb = jnp.where(s < 2, n2, pltpu.roll(n3, 4, 0))
    own = jnp.concatenate([t0a, t1a, t2a, t0b, t1b, t2b], axis=0)
    return own, jnp.concatenate([ha, hb], axis=0)


def token_regions(region_ids, levels):
    lines = jnp.repeat(region_ids, levels)
    pairs = lines.reshape(-1, 2)
    s = jnp.arange(3 * SUB)
    inner = s % SUB
    line0 = jnp.where(s < 8, 0, jnp.where(s < 16, 1, jnp.where((inner < 2) | (inner >= 6), 0, 1)))
    line1 = jnp.where(s < 8, 0, jnp.where(s < 16, 1, jnp.where((inner >= 2) & (inner < 6), 0, 1)))
    a, b = pairs[:, :1], pairs[:, 1:]
    both = jnp.stack([jnp.where(line0 == 0, a, b), jnp.where(line1 == 0, a, b)])
    per_band = WIN * levels // 2
    bands = pairs.shape[0] // per_band
    return both.reshape(2, bands, per_band * 3 * SUB).transpose(1, 0, 2)


def pack_kernel(f_ref, f_first, g_ref, g_first, low_ref, corner_ref, east_ref):
    n = low_ref.shape[1]
    for i, (x, first) in enumerate(((f_ref, f_first), (g_ref, g_first))):
        low_ref[i] = x[...]
        corner_ref[i] = first[:n]
        east_ref[i] = first[n:]


def pack(f_lines, g_lines, n):
    lines, cols, width = f_lines.shape
    low = pl.BlockSpec((n, cols, width), lambda i: (0, 0, 0))
    first = pl.BlockSpec((lines, SUB, width), lambda i: (0, 0, 0))
    shapes = [(2, n, cols, width), (2, n, SUB, width), (2, lines - n, SUB, width)]
    return pl.pallas_call(
        pack_kernel,
        grid=(1,),
        in_specs=[low, first, low, first],
        out_specs=[pl.BlockSpec(shape, lambda i: (0,) * 4) for shape in shapes],
        out_shape=tuple(jax.ShapeDtypeStruct(shape, BF16) for shape in shapes),
        name="pack",
    )(f_lines, f_lines, g_lines, g_lines)


def norm(block):
    centre = block - jnp.mean(block, axis=-1, keepdims=True)
    inverse = lax.rsqrt(jnp.mean(centre * centre, axis=-1, keepdims=True) + EPSILON)
    return (centre * inverse).astype(BF16), inverse


def put(at, p, block, grads, normed_ref, inv_ref, gs_ref):
    normed, inverse = norm(block)
    normed_ref[at, p] = normed
    inv_ref[at, p] = jnp.broadcast_to(inverse, (3 * SUB, LANES))
    gs_ref[at, p] = grads.astype(BF16)


def assemble_own_kernel(f_ref, g_ref, *outs):
    @pl.loop(0, f_ref.shape[0], unroll=9)
    def _(p):
        put(0, p, pick_first(f_ref[p].astype(F32)), pick_first(g_ref[p].astype(F32)), *outs)


def assemble_below_kernel(f_ref, g_ref, low_ref, *outs):
    @pl.when(pl.program_id(0) == 0)
    def _():
        @pl.loop(0, f_ref.shape[0], unroll=9)
        def _(p):
            put(0, p, pick_first(f_ref[p].astype(F32)), pick_first(g_ref[p].astype(F32)), *outs)

    @pl.when(pl.program_id(0) == 1)
    def _():
        @pl.loop(0, f_ref.shape[0], unroll=9)
        def _(p):
            put(0, p, pick_first(low_ref[0, p].astype(F32)), pick_first(low_ref[1, p].astype(F32)), *outs)


def assemble_second_kernel(f_ref, g_ref, east_ref, low_ref, corner_ref, *outs):
    last = pl.num_programs(0) - 1

    @pl.when(pl.program_id(0) < last)
    def _():
        @pl.loop(0, f_ref.shape[0], unroll=9)
        def _(p):
            put(
                0,
                p,
                pick_second(f_ref[p].astype(F32), east_ref[0, p].astype(F32)),
                pick_second(g_ref[p].astype(F32), east_ref[1, p].astype(F32)),
                *outs,
            )

    @pl.when(pl.program_id(0) == last)
    def _():
        @pl.loop(0, f_ref.shape[0], unroll=9)
        def _(p):
            put(
                0,
                p,
                pick_second(low_ref[0, p].astype(F32), corner_ref[0, p].astype(F32)),
                pick_second(low_ref[1, p].astype(F32), corner_ref[1, p].astype(F32)),
                *outs,
            )


def assembled(kernel, windows, skip, width, specs, args):
    shape = (windows, 2 * skip, 3 * SUB)
    out = lambda w: pl.BlockSpec((1, skip, 3 * SUB, w), lambda s: (s // 2, s % 2, 0, 0))
    outs = pl.pallas_call(
        kernel,
        grid=(2 * windows,),
        in_specs=specs,
        out_specs=[out(width), out(LANES), out(width)],
        out_shape=(
            jax.ShapeDtypeStruct(shape + (width,), BF16),
            jax.ShapeDtypeStruct(shape + (LANES,), F32),
            jax.ShapeDtypeStruct(shape + (width,), BF16),
        ),
        cost_estimate=pl.CostEstimate(
            flops=windows * skip * 3 * SUB * width * 100, transcendentals=0,
            bytes_accessed=windows * skip * 3 * SUB * width * 16),
        compiler_params=grant(30 if windows > 1 else None),
    )(*args)
    count = 2 * skip * 3 * SUB
    return [x.reshape(windows, count, x.shape[-1]) for x in outs]


def assemble_own(fields, grads, skip):
    width = fields.shape[2]
    own = pl.BlockSpec((skip, 48, width), lambda s: (s + 1, 0, 0))
    return assembled(assemble_own_kernel, 1, skip, width, [own, own], (fields, grads))


def assemble_below(fields, grads, low, skip):
    width = fields.shape[2]
    last = fields.shape[0] // skip - 1
    own = pl.BlockSpec((skip, 48, width), lambda s: (last, 0, 0))
    below = pl.BlockSpec((2, skip, 48, width), lambda s: (0, 0, 0, 0))
    return assembled(assemble_below_kernel, 1, skip, width, [own, own, below], (fields, grads, low))


def assemble_second(fields, grads, east, low, corner, skip):
    width = fields.shape[2]
    n = fields.shape[0] // skip - 1
    own = pl.BlockSpec((skip, 48, width), lambda s: (jnp.minimum(s + 1, n), 0, 0))
    strip = pl.BlockSpec((2, skip, 16, width), lambda s: (0, jnp.minimum(s, n - 1), 0, 0))
    below = pl.BlockSpec((2, skip, 48, width), lambda s: (0, 0, 0, 0))
    diagonal = pl.BlockSpec((2, skip, 16, width), lambda s: (0, 0, 0, 0))
    return assembled(
        assemble_second_kernel, (n + 1) // 2, skip, width, [own, own, strip, below, diagonal],
        (fields, grads, east, low, corner),
    )


def attention_kernel(*refs, carried, last):
    normed_ref, inv_ref, gs_ref, reg_ref, w_ref, wp_ref = refs[:6]
    refs = refs[6:]
    gw_in = gp_in = None
    if carried:
        gw_in, gp_in = refs[:2]
        refs = refs[2:]
    back_ref, gw_ref, gp_ref, branch_acc, pre_acc = refs
    group = pl.program_id(0)
    window = pl.program_id(1)
    scale = HEAD ** (-0.5)
    normed = normed_ref[window]
    grads = gs_ref[window]
    count = normed.shape[0]
    wide = GROUP * LANES
    weights = w_ref[...].reshape(3 * wide, w_ref.shape[2])
    qkv = nt(normed, weights).astype(BF16)
    queries, all_keys, all_values = [qkv[:, wide * i : wide * (i + 1)] for i in range(3)]
    queries = queries * jnp.asarray(scale, BF16)
    grad_att_all = nn(grads, wp_ref[...]).astype(BF16)
    all_keys_t = all_keys.astype(F32).T.astype(BF16) * jnp.asarray(scale, BF16)
    all_values_t = all_values.astype(F32).T.astype(BF16)
    region = reg_ref[window]
    region_t = jnp.broadcast_to(region, (LANES, count)).T
    spread = jnp.concatenate([region_t] * -(-count // LANES), axis=1)[:, :count]
    allowed = spread == region
    lane = lax.broadcasted_iota(jnp.int32, (count, LANES), 1)
    zero = jnp.zeros((), BF16)
    heads = GROUP * LANES // HEAD
    pairs = LANES // HEAD

    def inputs(h):
        pair, k = divmod(h, pairs)
        cols = slice(pair * LANES, (pair + 1) * LANES)
        mine = (lane >= k * HEAD) & (lane < (k + 1) * HEAD)
        return cols, lambda x: jnp.where(mine, x[:, cols], zero)

    def products(h):
        cols, only = inputs(h)
        scores = nt(only(all_keys), queries[:, cols])
        return jnp.where(allowed, scores, -1e30), nt(only(all_values), grad_att_all[:, cols])

    def softmax(scores, grad_probs):
        peak = jnp.max(scores, axis=0, keepdims=True)
        expo = jnp.exp(scores - peak)
        ratio = 1.0 / jnp.sum(expo, axis=0, keepdims=True)
        rounded = (expo * ratio).astype(BF16)
        inner = jnp.sum(grad_probs * expo, axis=0, keepdims=True) * ratio
        return rounded, (expo * (grad_probs - inner) * ratio).astype(BF16)

    def gradients(h, rounded, grad_scores):
        _, only = inputs(h)
        rows = slice(h * HEAD, (h + 1) * HEAD)
        return (
            nn(all_values_t[rows], rounded),
            nn(all_keys_t[rows], grad_scores),
            nn(grad_scores, only(queries)),
            nn(rounded, only(grad_att_all)),
        )

    def joined(k, first, number):
        return jnp.concatenate([d[k] for d in done[first * pairs : (first + number) * pairs]], axis=0)

    def att_rows(first, number):
        return joined(0, first, number).T.astype(BF16)

    def back_to_rows(first, number):
        return joined(1, first, number).T.astype(BF16)

    def key_and_value(first, number, turned=False):
        out = []
        for k in (2, 3):
            both = [
                sum(d[k] for d in done[p * pairs : (p + 1) * pairs]) for p in range(first, first + number)
            ]
            if turned:
                out.append(jnp.concatenate([x.T.astype(BF16) for x in both], axis=0))
            else:
                out.append(jnp.concatenate([x.astype(BF16) for x in both], axis=1))
        return out

    def sums(first, number):
        turned = [joined(1, first, number).astype(BF16), *key_and_value(first, number, True)]
        grad_w = nn(jnp.concatenate(turned, axis=0), normed)
        grad_w = grad_w.reshape(3, number * LANES, grad_w.shape[1])
        return grad_w, nn(joined(0, first, number).astype(BF16), grads).T, first

    ahead, weights_of, done = {0: products(0)}, {}, []
    parts = [(0, GROUP)]
    early = {}
    for h in range(heads + 1):
        if h + 1 < heads:
            ahead[h + 1] = products(h + 1)
        if h < heads:
            weights_of[h] = softmax(*ahead.pop(h))
        if h > 0:
            done.append(gradients(h - 1, *weights_of.pop(h - 1)))
    att = att_rows(0, GROUP)
    grad_qkv = jnp.concatenate([back_to_rows(0, GROUP), *key_and_value(0, GROUP)], axis=1)
    branch = nt(att, wp_ref[...])
    grad_normed = nn(grad_qkv, weights)
    started = group > 0
    branch += jnp.where(started, branch_acc[window], 0.0)
    grad_normed += jnp.where(started, pre_acc[window], 0.0)
    branch_acc[window] = branch
    pre_acc[window] = grad_normed
    back_ref[0, 0] = branch.astype(BF16)
    normal = normed.astype(F32)
    mean = jnp.mean(grad_normed, axis=-1, keepdims=True)
    along = jnp.mean(grad_normed * normal, axis=-1, keepdims=True)
    pre = inv_ref[window][:, :1] * (grad_normed - mean - normal * along)
    back_ref[0, 1] = pre.astype(BF16)
    opening = window == 0
    kind = gw_ref.dtype
    for pairs_of in parts:
        grad_w, grad_p, at = sums(*pairs_of) if pairs_of not in early else early[pairs_of]
        cols = pl.ds(at * LANES, grad_p.shape[1])
        for ref, mine, carry, where in (
            (gw_ref, grad_w, gw_in, (slice(None), cols)),
            (gp_ref, grad_p, gp_in, (slice(None), cols)),
        ):
            if last:
                ref[where] = (mine + carry[where] if carried else mine).astype(kind)
            else:
                base = carry[where] if carried else 0.0
                ref[where] = mine + jnp.where(opening, base, ref[where])


def attention(normed, inv, gs, regions, w_qkv, w_proj, carry=(), last=False):
    windows, count, width = normed.shape
    assert not last or windows == 1
    wide = GROUP * LANES
    number = width // wide
    whole = lambda *shape: pl.BlockSpec(shape, lambda p, w: (0,) * len(shape))
    rows3 = pl.BlockSpec((3, wide, width), lambda p, w: (0, p, 0))
    cols1 = pl.BlockSpec((width, wide), lambda p, w: (0, p))
    kind = BF16 if last else F32
    return pl.pallas_call(
        functools.partial(attention_kernel, carried=bool(carry), last=last),
        grid=(number, windows),
        in_specs=[
            whole(windows, count, width),
            whole(windows, count, LANES),
            whole(windows, count, width),
            whole(windows, 1, count),
            rows3,
            cols1,
        ]
        + ([rows3, cols1] if carry else []),
        out_specs=[
            pl.BlockSpec(
                (1, 2, count, width), lambda p, w: (jnp.where(p == number - 1, w, 0), 0, 0, 0)
            ),
            rows3,
            cols1,
        ],
        out_shape=(
            jax.ShapeDtypeStruct((windows, 2, count, width), BF16),
            jax.ShapeDtypeStruct((3, width, width), kind),
            jax.ShapeDtypeStruct((width, width), kind),
        ),
        scratch_shapes=[pltpu.VMEM((windows, count, width), F32)] * 2,
        input_output_aliases={6: 1, 7: 2} if carry and not last else {},
        cost_estimate=pl.CostEstimate(
            flops=windows * count * width * (20 * width + 12 * count), transcendentals=0,
            bytes_accessed=windows * count * width * 12),
        compiler_params=grant(30),
    )(normed, inv, gs, regions[:, None, :], w_qkv, w_proj, *carry)


def send_kernel(below, second, east, f_ref, g_ref, out_ref, gout_ref, east0, east1, low_ref,
                corner_ref):
    n = f_ref.shape[0]

    @pl.loop(0, n, unroll=3)
    def _(p):
        for i in range(2):
            tokens = east[0, i, p].astype(F32)
            east0[i, p] = unpick(tokens, tokens)[1].astype(BF16)

    @pl.when(pl.program_id(0) == 0)
    def _():
        @pl.loop(0, n, unroll=3)
        def _(p):
            for i, (x, o) in enumerate(((f_ref, out_ref), (g_ref, gout_ref))):
                add, strip = unpick(below[0, i, p].astype(F32), second[0, i, p].astype(F32))
                o[p] = (x[p].astype(F32) + add).astype(BF16)
                east1[i, p] = strip.astype(BF16)

    @pl.when(pl.program_id(0) == 1)
    def _():
        @pl.loop(0, n, unroll=3)
        def _(p):
            for i in range(2):
                add, strip = unpick(below[0, i, p].astype(F32), second[0, i, p].astype(F32))
                low_ref[i, p] = add.astype(BF16)
                corner_ref[i, p] = strip.astype(BF16)


def send(below, second, fields, grads, skip):
    pairs, _, width = fields.shape
    last = pairs // skip - 1
    own = pl.BlockSpec((skip, 48, width), lambda s: (last, 0, 0))
    half = lambda at: pl.BlockSpec((1, 2, skip, 3 * SUB, width), lambda s: (at, 0, s, 0, 0))
    whole = lambda *shape: pl.BlockSpec(shape, lambda s: (0,) * len(shape))
    strips = [(2, skip, 16, width), (2, skip, 48, width), (2, skip, 16, width)]
    outs = [(pairs, 48, width)] * 2 + [(2, 2 * skip, 16, width)] + strips
    return pl.pallas_call(
        send_kernel,
        grid=(2,),
        in_specs=[half(0), half(1), half(0), own, own],
        out_specs=[own, own, pl.BlockSpec((2, skip, 16, width), lambda s: (0, s, 0, 0))]
        + [whole(*shape) for shape in strips],
        out_shape=tuple(jax.ShapeDtypeStruct(shape, BF16) for shape in outs),
        compiler_params=grant(20),
        name="send",
    )(below, second, second, fields, grads)


def finish_kernel(first, second, f_ref, g_ref, any0, any1, out_ref, gout_ref):
    @pl.loop(0, f_ref.shape[0], unroll=3)
    def _(p):
        for i, (x, o) in enumerate(((f_ref, out_ref), (g_ref, gout_ref))):
            add, _ = unpick(first[0, i, p].astype(F32), second[0, i, p].astype(F32))
            o[p] = (x[p].astype(F32) + add).astype(BF16)


def finish(first, second, fields, grads, skip, out, gout):
    pairs, _, width = fields.shape
    own = pl.BlockSpec((skip, 48, width), lambda s: (s + 1, 0, 0))
    anyw = pl.BlockSpec(memory_space=pl.ANY)
    half = pl.BlockSpec((1, 2, skip, 3 * SUB, width), lambda s: (0, 0, s, 0, 0))
    return pl.pallas_call(
        finish_kernel,
        grid=(2,),
        in_specs=[half, half, own, own, anyw, anyw],
        out_specs=[own, own],
        out_shape=(jax.ShapeDtypeStruct((pairs, 48, width), BF16),) * 2,
        input_output_aliases={4: 0, 5: 1},
        compiler_params=grant(20),
        name="finish",
    )(first, second, fields, grads, out, gout)


def edge_kernel(f_ref, o_ref, r_ref, g_ref, q_ref, out_ref, gout_ref):
    s = lax.broadcasted_iota(jnp.int32, f_ref.shape, 1)
    for i, (f, o, out) in enumerate(((f_ref, o_ref, out_ref), (g_ref, q_ref, gout_ref))):
        total = f[...].astype(F32) + r_ref[i].astype(F32)
        out[...] = jnp.where(s < HALF, total, o[...].astype(F32)).astype(BF16)


def edge(fields, out, back, grads, gout, skip, first):
    _, _, width = fields.shape
    n = back.shape[1] // skip
    at = pl.BlockSpec((skip, SUB, width), lambda i: (i + first, 0, 0))
    strip = pl.BlockSpec((2, skip, SUB, width), lambda i: (0, i, 0, 0))
    return pl.pallas_call(
        edge_kernel,
        grid=(n,),
        in_specs=[at, at, strip, at, at],
        out_specs=[at, at],
        out_shape=(jax.ShapeDtypeStruct(out.shape, BF16),) * 2,
        input_output_aliases={1: 0, 4: 1},
        name="edge",
    )(fields, out, back, grads, gout)


def rim_kernel(f_ref, low_ref, c_ref, g_ref, out_any, gout_any, out_ref, gout_ref):
    for i, (f, out) in enumerate(((f_ref, out_ref), (g_ref, gout_ref))):
        back = low_ref[i].astype(F32)
        corner = c_ref[i].astype(F32)
        s = lax.broadcasted_iota(jnp.int32, corner.shape, 1)
        head = jnp.where(s < HALF, corner, back[:, :SUB])
        back = jnp.concatenate([head, back[:, SUB:]], axis=1)
        out[...] = (f[...].astype(F32) + back).astype(BF16)


def rim(fields, low, corner, grads, out, gout):
    _, skip, cols, width = low.shape
    at = pl.BlockSpec((skip, cols, width), lambda i: (0, 0, 0))
    whole = lambda *shape: pl.BlockSpec(shape, lambda i: (0,) * len(shape))
    anyw = pl.BlockSpec(memory_space=pl.ANY)
    return pl.pallas_call(
        rim_kernel,
        grid=(1,),
        in_specs=[at, whole(2, skip, cols, width), whole(2, skip, SUB, width), at, anyw, anyw],
        out_specs=[at, at],
        out_shape=(jax.ShapeDtypeStruct(out.shape, BF16),) * 2,
        input_output_aliases={4: 0, 5: 1},
        name="rim",
    )(fields, low, corner, grads, out, gout)


def linear(lon, lat, lats):
    return lon * lats + lat


def shift_by(block, step_lon, step_lat):
    lons, lats = lax.axis_size("lon"), lax.axis_size("lat")
    route = [
        (linear((i + step_lon) % lons, (j + step_lat) % lats, lats), linear(i, j, lats))
        for i in range(lons)
        for j in range(lats)
    ]
    return lax.ppermute(block, AXES, route)


def stages():
    lons, lats = lax.axis_size("lon"), lax.axis_size("lat")
    lat_bits = [1 << i for i in range(lats.bit_length() - 1)]
    lon_bits = [lats << i for i in range(lons.bit_length() - 1)]
    assert lats == 1 << len(lat_bits) and lons == 1 << len(lon_bits)
    far = lon_bits[1:]
    groups = [lat_bits[i : i + 2] for i in range(0, len(lat_bits), 2)]
    groups += [far[i : i + 2] for i in range(0, len(far), 2)]
    groups += [lon_bits[:1]]
    return groups, sorted(lat_bits + lon_bits)[::-1]


def swap(block, bit):
    total = lax.axis_size("lon") * lax.axis_size("lat")
    return lax.ppermute(block, AXES, [(i, i ^ bit) for i in range(total)])


def join(mine, other, bit, bits, place):
    high = (place & bit) != 0
    axis = bits.index(bit)
    return jnp.where(
        high,
        jnp.concatenate([other, mine], axis=axis),
        jnp.concatenate([mine, other], axis=axis),
    )


def gather_stage(held, group, bits, place):
    if len(group) == 1:
        return join(held, swap(held, group[0]), group[0], bits, place)
    b1, b2 = group
    o1, o2, o3 = swap(held, b1), swap(held, b2), swap(held, b1 | b2)
    return join(join(held, o1, b1, bits, place), join(o2, o3, b1, bits, place), b2, bits, place)


def part_of(held, bit, bits, index):
    return lax.dynamic_index_in_dim(held, index, bits.index(bit), keepdims=True)


def scatter_terms(held, group, bits, place):
    here = [jnp.where((place & bit) != 0, 1, 0) for bit in group]
    own = held
    for bit, i in zip(group, here):
        own = part_of(own, bit, bits, i)
    terms = [own]
    for flips in range(1, 1 << len(group)):
        send, mask = held, 0
        for k, (bit, i) in enumerate(zip(group, here)):
            flip = (flips >> k) & 1
            send = part_of(send, bit, bits, 1 - i if flip else i)
            mask |= bit * flip
        terms.append(swap(send.astype(BF16), mask))
    return terms


def last_join_kernel(place_ref, mine_ref, other_ref, w_ref, p_ref):
    share = w_ref.shape[3]
    for own, ref in ((True, mine_ref), (False, other_ref)):
        at = place_ref[0] if own else 1 - place_ref[0]
        w_ref[:, at] = ref[:, :, :share]
        p_ref[:, at] = ref[:, :, share:]


def last_join(mine, other, place, share):
    far, near, rows, width = mine.shape
    whole = lambda *shape: pl.BlockSpec(shape, lambda i, p: (0,) * len(shape))
    shapes = [(far, 2, near, share, width), (far, 2, near, rows - share, width)]
    return pl.pallas_call(
        last_join_kernel,
        grid_spec=pltpu.PrefetchScalarGridSpec(
            num_scalar_prefetch=1,
            grid=(1,),
            in_specs=[whole(*mine.shape)] * 2,
            out_specs=[whole(*shape) for shape in shapes],
        ),
        out_shape=tuple(jax.ShapeDtypeStruct(shape, BF16) for shape in shapes),
        name="last_join",
    )(place, mine, other)


def lines_of(grid):
    rows, cols, levels, width = grid.shape
    return grid.transpose(0, 2, 1, 3).reshape(rows * levels, cols, width)


def grid_of(lines, levels):
    count, cols, width = lines.shape
    return lines.reshape(count // levels, levels, cols, width).transpose(0, 2, 1, 3)


def paired(lines):
    *lead, count, cols, width = lines.shape
    return lines.reshape(*lead, count // 2, 2 * cols, width)


def unpaired(pairs):
    *lead, count, cols, width = pairs.shape
    return pairs.reshape(*lead, count * 2, cols // 2, width)


def block(fields, region_ids, w_qkv, w_proj, grad_output):
    rows, cols, levels, width = fields.shape
    skip = HALF * levels // 2
    devices = lax.axis_size("lon") * lax.axis_size("lat")
    factor = float(rows * cols * levels * devices) ** (-0.5)
    place = lax.axis_index(AXES)
    groups, bits = stages()
    share = w_qkv.shape[0]
    f_lines, g_lines = lines_of(fields), lines_of(grad_output)
    f_pairs, g_pairs = paired(f_lines), paired(g_lines)
    held = jnp.concatenate([w_qkv, w_proj], axis=0)
    held = held.reshape((1,) * len(bits) + held.shape)
    for group in groups[:-1]:
        held = gather_stage(held, group, bits, place)
    bit = groups[-1][0]
    held = lax.optimization_barrier(held)
    other = swap(held, bit)
    near = bit
    halves = [x.reshape(-1, near, held.shape[-2], width) for x in (held, other)]
    w3, p_all = last_join(*halves, jnp.where((place & bit) != 0, 1, 0).reshape(1), share)
    w3, p_all = w3.reshape(3, width, width), p_all.reshape(width, width)
    low, corner, east = pack(f_lines, g_lines, 2 * skip)
    low = shift_by(low, 0, 1)
    east = shift_by(east, 1, 0)
    corner = shift_by(corner, 1, 1)
    low, east, corner = paired(low), paired(east), paired(corner)
    regions = token_regions(region_ids, levels)
    n00, i00, g00 = assemble_own(f_pairs, g_pairs, skip)
    n10, i10, g10 = assemble_below(f_pairs, g_pairs, low, skip)
    b10, *carry = attention(n10, i10, g10, regions[1, :1], w3, p_all)
    n1, i1, g1 = assemble_second(f_pairs, g_pairs, east, low, corner, skip)
    b1, *carry = attention(n1, i1, g1, regions[:, 1], w3, p_all, carry)
    b10, b1 = [x.reshape(-1, 2, 2 * skip, 3 * SUB, width) for x in (b10, b1)]
    out, gout, r_east0, r_east1, r_low, r_corner = send(b10, b1, f_pairs, g_pairs, skip)
    r_low = shift_by(unpaired(r_low), 0, -1)
    r_corner = shift_by(unpaired(r_corner), -1, -1)
    r_east1 = shift_by(unpaired(r_east1), -1, 0)
    r_east0 = shift_by(unpaired(r_east0), -1, 0)
    b00, grad_w, grad_p = attention(n00, i00, g00, regions[0, :1], w3, p_all, carry, True)
    b00 = b00.reshape(-1, 2, 2 * skip, 3 * SUB, width)
    grads = jnp.concatenate(
        [grad_w.reshape(devices, -1, width), grad_p.reshape(devices, -1, width)], axis=1
    )
    grads = grads.reshape((2,) * len(bits) + grads.shape[1:])
    for i, group in enumerate(groups[::-1]):
        terms = scatter_terms(grads, group, bits, place)
        if i + 1 < len(groups):
            grads = sum(x.astype(F32) for x in terms)
    terms = [x.reshape(-1, width) for x in terms]
    grad_w = sum(x[:share].astype(F32) for x in terms) * factor
    grad_p = sum(x[share:].astype(F32) for x in terms) * factor
    out, gout = finish(b00, b1, f_pairs, g_pairs, skip, out, gout)
    out, gout = unpaired(out), unpaired(gout)
    out, gout = rim(f_lines, r_low, r_corner, g_lines, out, gout)
    out, gout = edge(f_lines, out, r_east1, g_lines, gout, 2 * skip, rows * levels // (2 * skip) - 1)
    out, gout = edge(f_lines, out, r_east0, g_lines, gout, 2 * skip, 1)
    return (grid_of(out, levels), grid_of(gout, levels), grad_w, grad_p)


def solution(mesh):
    return jax.shard_map(
        block,
        mesh=mesh,
        in_specs=(
            P("lat", "lon", None, None),
            P("lat"),
            P(AXES, None),
            P(AXES, None),
            P("lat", "lon", None, None),
        ),
        out_specs=(
            P("lat", "lon", None, None),
            P("lat", "lon", None, None),
            P(AXES, None),
            P(AXES, None),
        ),
        check_vma=False,
    )
```
